128 devices in a mesh: lat: 8 (over y_hi, x), lon: 16 (over z, y_lo, core).
Axes of the slice: x: 4, y: 4 (y_hi: 2, y_lo: 2; y = y_hi * 2 + y_lo), z: 4, core: 2. Of those that a mesh axis runs over, the one named last changes fastest.
Arguments:
- state: float32 [8, 60, 64, 2048], P(None, None, 'lat', 'lon'), may hold values from -6 to 6
- surface: bfloat16 [76, 64, 2048], P(None, 'lat', 'lon'), may hold values from -6 to 6
- layer_one: bfloat16 [556, 768], replicated, may hold values from -0.25 to 0.25
- layer_two: bfloat16 [768, 640], replicated, may hold values from -0.21875 to 0.21875
- layer_three: bfloat16 [640, 512], replicated, may hold values from -0.25 to 0.25
- layer_four: bfloat16 [512, 640], replicated, may hold values from -0.25 to 0.25
- layer_five: bfloat16 [640, 368], replicated, may hold values from -0.25 to 0.25
- lit_columns: int32 [8, 16, 1024], P('lat', 'lon'), may hold values from 0 to 1024, as said below
- row_offset: int32 [64], P('lat'), may hold values from 0 to 383
Outputs:
- new_state: float32 [8, 60, 64, 2048], P(None, None, 'lat', 'lon')
- surface_flux: bfloat16 [8, 64, 2048], P(None, 'lat', 'lon')
The draws below stay inside these ranges and needn't reach their ends.
Inputs may be any that keep to these rules, and one draw needn't show every extreme that they name: `lit_columns`: in each tile's list the first entries are distinct column numbers in rising order and the rest equal 1024. A tile and the tile 16/2 further along the longitude cycle, in the same latitude tile, list 1024 columns together at most, and some such pair lists exactly 1024 in every draw.
All inputs are finite; a program needn't handle non-finite values.
Results may differ from the reference program's by a relative error of at most 0.015.
Values may be sent and summed in bfloat16 or wider, within the bound.
A program may use at most 64 MiB of HBM per device.

```python
import jax
import jax.numpy as jnp
from jax import lax

CLAT = 8
CLON = 128
LEV = 60
SUBSTEPS = 4
REACH = 2
NSURF = 76
NFLUX = 8
H1 = 768
H2 = 640
H3 = 512
H4 = 640
NIN = 556
NOUT = 368
CPT = 1024
HALF = 512
NLAT = 64
NLON = 2048
N_LAT = 8
N_LON = 16


def draw_lit_columns(key, part):
    key_total, key_share, key_full, key_sun, key_perm = jax.random.split(jax.random.fold_in(key, 11), 5)
    half_cycle = N_LON // 2
    pair_total = jax.random.randint(key_total, (N_LAT, half_cycle), CPT // 2, CPT + 1)
    full_pair = jax.random.randint(key_full, (), 0, N_LAT * half_cycle)
    pair_total = pair_total.reshape(-1).at[full_pair].set(CPT).reshape(N_LAT, half_cycle)
    night_count = jax.random.randint(key_share, (N_LAT, half_cycle), 0, pair_total // 4 + 1)
    day_count = pair_total - night_count
    sun_place = jax.random.randint(key_sun, (), 0, N_LON)
    first_half = jnp.arange(half_cycle, dtype=jnp.int32)
    first_lit = (first_half - sun_place) % N_LON < half_cycle
    first_count = jnp.where(first_lit[None, :], day_count, night_count)
    second_count = jnp.where(first_lit[None, :], night_count, day_count)
    counts = jnp.concatenate([first_count, second_count], axis=1)
    tile_keys = jax.random.split(key_perm, N_LAT * N_LON)
    shuffled = jax.vmap(lambda tile_key: jax.random.permutation(tile_key, CPT))(tile_keys).reshape(N_LAT, N_LON, CPT)
    position = jnp.arange(CPT, dtype=jnp.int32)
    chosen = jnp.where(position[None, None, :] < counts[:, :, None], shuffled, CPT)
    return jnp.sort(chosen, axis=-1).astype(jnp.int32)


def set_ends(values, key, smallest, largest):
    dims = values.shape
    spot = [jax.random.randint(jax.random.fold_in(key, axis), (), 0, dims[axis]) for axis in range(len(dims))]
    values = values.at[tuple(spot)].set(smallest)
    longest = dims.index(max(dims))
    spot[longest] = (spot[longest] + 1) % dims[longest]
    return values.at[tuple(spot)].set(largest)


def level_of(rng, shape, cuts, smallest, high):
    def one(axis_at, parts):
        heights = jax.random.uniform(jax.random.fold_in(jax.random.fold_in(rng, 6), axis_at), (parts,), jnp.float32, smallest / len(cuts), high / len(cuts))
        return jnp.repeat(jnp.exp(heights), shape[axis_at] // parts).reshape((-1,) + (1,) * (len(shape) - axis_at - 1))

    factor_of = one(*cuts[0])
    for cut in cuts[1:]:
        factor_of = factor_of * one(*cut)
    return factor_of


def bell_draw(own_key, extent, spread, limit, shards=(), held_as=jnp.bfloat16):
    gain = level_of(own_key, extent, shards, -0.22, 0.18) if shards else 1.0
    array = jax.random.normal(own_key, extent, jnp.float32) * spread * gain
    return jnp.minimum(jnp.maximum(array, -limit), limit).astype(held_as)


def setup_inputs(seed: int = 0) -> dict:
    arg_keys = jax.random.split(jax.random.key(seed), 10)
    return {
        "state": bell_draw(arg_keys[0], (8, LEV, NLAT, NLON), 1.0, 6.0, ((2, 8), (3, 16)), jnp.float32),
        "surface": bell_draw(arg_keys[1], (NSURF, NLAT, NLON), 1.0, 6.0, ((1, 8), (2, 16))),
        "layer_one": bell_draw(arg_keys[2], (NIN, H1), NIN ** -0.5, 0.25),
        "layer_two": bell_draw(arg_keys[3], (H1, H2), H1 ** -0.5, 0.21875),
        "layer_three": bell_draw(arg_keys[4], (H2, H3), H2 ** -0.5, 0.25),
        "layer_four": bell_draw(arg_keys[5], (H3, H4), H3 ** -0.5, 0.25),
        "layer_five": bell_draw(arg_keys[6], (H4, NOUT), H4 ** -0.5, 0.25),
        "lit_columns": draw_lit_columns(jax.random.fold_in(arg_keys[9], 71), 0),
        "row_offset": set_ends(jax.random.randint(arg_keys[8], (NLAT,), 0, (REACH + 1) * CLON), jax.random.fold_in(arg_keys[8], 1), 0, ((REACH + 1) * CLON) - 1).astype(jnp.int32),
    }


SOUND_COURANT = 0.6
PHYSICS_STEP = 0.5
LEAK_SLOPE = 0.15


def run_network(inputs, layers):
    hidden = inputs
    for weight in layers[:-1]:
        summed = lax.dot_general(weight, hidden, (((0,), (0,)), ((), ())), preferred_element_type=jnp.float32)
        hidden = jnp.maximum(summed, LEAK_SLOPE * summed).astype(jnp.bfloat16)
    summed = lax.dot_general(layers[-1], hidden, (((0,), (0,)), ((), ())), preferred_element_type=jnp.float32)
    return summed.astype(jnp.bfloat16)


def mark_lit(listing):
    return jnp.zeros((CPT + 1,), jnp.float32).at[listing].set(1.0)[:CPT]


def reference(state, surface, layer_one, layer_two, layer_three, layer_four, layer_five, lit_columns, row_offset):
    zonal_wind, merid_wind, pressure = state[0], state[1], state[2]
    lat_rows = jnp.arange(NLAT, dtype=jnp.int32)
    north_open = (lat_rows < NLAT - 1).astype(jnp.float32)[None, :, None]
    for substep in range(SUBSTEPS):
        zonal_wind = zonal_wind - SOUND_COURANT * (jnp.roll(pressure, -1, axis=2) - pressure)
        north_row = jnp.concatenate([pressure[:, 1:], jnp.zeros_like(pressure[:, :1])], axis=1)
        merid_wind = (merid_wind - SOUND_COURANT * (north_row - pressure)) * north_open
        south_row = jnp.concatenate([jnp.zeros_like(merid_wind[:, :1]), merid_wind[:, :-1]], axis=1)
        pressure = pressure - SOUND_COURANT * (zonal_wind - jnp.roll(zonal_wind, 1, axis=2) + merid_wind - south_row)
    all_columns = NLAT * NLON
    dynamics = jnp.stack([zonal_wind, merid_wind, pressure]).reshape(3 * LEV, all_columns)
    features = jnp.concatenate([dynamics, state[3:].reshape(5 * LEV, all_columns), surface.astype(jnp.float32).reshape(NSURF, all_columns)], axis=0).astype(jnp.bfloat16)
    lit_mask = jax.vmap(jax.vmap(mark_lit))(lit_columns)
    lit_mask = lit_mask.reshape(N_LAT, N_LON, CLAT, CLON).transpose(0, 2, 1, 3).reshape(all_columns)
    lit_index = jnp.nonzero(lit_mask > 0.5, size=all_columns // 2, fill_value=all_columns)[0].astype(jnp.int32)
    picked = jnp.take(features, jnp.minimum(lit_index, all_columns - 1), axis=1)
    batches = picked.reshape(NIN, all_columns // 2 // HALF, HALF).transpose(1, 0, 2)
    layers = (layer_one, layer_two, layer_three, layer_four, layer_five)
    physics_out = lax.map(lambda batch: run_network(batch, layers), batches)
    physics_out = physics_out.transpose(1, 0, 2).reshape(NOUT, all_columns // 2)
    results = jnp.zeros((NOUT, all_columns + 1), jnp.bfloat16).at[:, lit_index].set(physics_out)[:, :all_columns]
    tendency = results[:6 * LEV].astype(jnp.float32).reshape(6, LEV, NLAT, NLON)
    surface_flux = results[6 * LEV:].reshape(NFLUX, NLAT, NLON)
    updated_zonal = zonal_wind + PHYSICS_STEP * tendency[0]
    updated_merid = merid_wind + PHYSICS_STEP * tendency[1]
    scalars = state[3:] + PHYSICS_STEP * jnp.concatenate([tendency[2:], jnp.zeros_like(tendency[:1])], axis=0)
    fraction = 0.5 + 0.45 * jnp.tanh(zonal_wind)
    fraction_west = jnp.roll(fraction, 1, axis=2)
    source_index = (jnp.arange(NLON, dtype=jnp.int32)[None, :] - row_offset[:, None]) % NLON

    def advect(tracer):
        near_index = jnp.broadcast_to(source_index, tracer.shape)
        far_index = (near_index - 1) % NLON
        near_value = jnp.take_along_axis(tracer, near_index, axis=2)
        far_value = jnp.take_along_axis(tracer, far_index, axis=2)
        return (1.0 - fraction) * near_value + fraction_west * far_value

    advected = lax.map(advect, scalars)
    new_state = jnp.concatenate([jnp.stack([updated_zonal, updated_merid, pressure]), advected], axis=0)
    return new_state, surface_flux
```

```python
import jax
import jax.numpy as jnp
from jax import lax
from jax.experimental import pallas as pl
from jax.experimental.pallas import tpu as pltpu
from jax.sharding import PartitionSpec as P

MESH = pl.DeviceIdType.MESH
F32, BF16 = jnp.float32, jnp.bfloat16

N_LAT, N_LON = 8, 16
LEV = 60
ROWS, COLS = 8, 128
FIELD = LEV * ROWS
COURANT = 0.6
STEP = 0.5
SLOPE = 0.15
DYN = 192
NIN, NOUT = 556, 368
H1, H2, H3, H4 = 768, 640, 512, 640

LC = 20
NCH = LEV // LC
HC = LC // 2
PER = 10
GROUPS = LEV // PER
CH = 2
NB = ROWS // CH
OZ = NB

EDGES = ((0, -1), (0, 1), (-1, -1), (-1, 1), (1, -1), (1, 1))


def nt(a, b):
    return lax.dot_general(a, b, (((1,), (1,)), ((), ())), preferred_element_type=F32)


def eye(n):
    return (lax.broadcasted_iota(jnp.int32, (n, n), 0) == lax.broadcasted_iota(jnp.int32, (n, n), 1)).astype(F32).astype(BF16)


def leaky(z):
    return jnp.maximum(z, SLOPE * z).astype(BF16)


def kernel(
    state, surface, w1h, w2h, w3h, w4h, w5h, lith, off,
    out, flux,
    st, sfb, sf, w1, w2, w3, w4, w5t, lit, acc, mask, fr, fw, fl,
    rsend, rrecv, esend, erecv, ca, cb, oz, qb,
    load_sem, rs_sem, rr_sem, es_sem, er_sem, qs_sem, qr_sem,
):
    lat, lon = lax.axis_index("lat"), lax.axis_index("lon")
    core, quarter = lax.rem(lon, 2), lax.rem(lon, 4)

    def at(dlat, dlon):
        return (lat + dlat, lax.rem(lon + dlon + N_LON, N_LON))

    loads = [
        pltpu.make_async_copy(state.at[0 : 3 * FIELD], st.at[0 : 3 * FIELD], load_sem.at[0]),
        pltpu.make_async_copy(state.at[3 * FIELD : 8 * FIELD], st.at[3 * FIELD : 8 * FIELD], load_sem.at[1]),
        pltpu.make_async_copy(surface, sfb, load_sem.at[2]),
        pltpu.make_async_copy(lith, lit, load_sem.at[3]),
        pltpu.make_async_copy(w1h, w1, load_sem.at[4]),
        pltpu.make_async_copy(w5h, w5t, load_sem.at[5]),
        pltpu.make_async_copy(w2h, w2, load_sem.at[6]),
        pltpu.make_async_copy(w3h, w3, load_sem.at[7]),
        pltpu.make_async_copy(w4h, w4, load_sem.at[8]),
    ]
    for load in loads:
        load.start()

    barrier = pltpu.get_barrier_semaphore()

    def greet(dlat, dlon):
        pl.semaphore_signal(barrier, inc=1, device_id=at(dlat, dlon), device_id_type=MESH)

    for dlon in (-3, -2, -1, 1, 2, 3):
        greet(0, dlon)

    @pl.when(lat > 0)
    def _():
        for dlon in (-1, 0, 1):
            greet(-1, dlon)

    @pl.when(lat < N_LAT - 1)
    def _():
        for dlon in (-1, 0, 1):
            greet(1, dlon)

    loads[0].wait()
    sub3 = lax.broadcasted_iota(jnp.int32, (HC, ROWS, COLS), 1) < 4
    for ch in range(NCH):
        for f in range(3):
            x = st[f * FIELD + ch * LC * ROWS : f * FIELD + (ch + 1) * LC * ROWS].reshape(LC, ROWS, COLS)
            low, high = x[:HC], x[HC:]
            to_south = jnp.where(sub3, low, pltpu.roll(high, 4, 1))
            to_north = jnp.where(sub3, pltpu.roll(low, 4, 1), high)
            spot = slice(f * HC * ROWS, (f + 1) * HC * ROWS)
            rsend[0, ch, spot] = to_south.reshape(HC * ROWS, COLS).astype(BF16)
            rsend[1, ch, spot] = to_north.reshape(HC * ROWS, COLS).astype(BF16)
    lane2 = lax.broadcasted_iota(jnp.int32, (ROWS, COLS), 1)
    packed = []
    for f in range(3):
        for g in range(GROUPS):
            total = jnp.zeros((ROWS, COLS), F32)
            for kk in range(PER):
                row = (f * LEV + g * PER + kk) * ROWS
                total = jnp.where(lane2 // 8 == kk, pltpu.roll(st[row : row + ROWS], 4 + 8 * kk, 1), total)
            packed.append(total)
    esend[...] = jnp.concatenate(packed, axis=0).astype(BF16)

    neighbours = 6 + 3 * ((lat + N_LAT - 1) // N_LAT) + 3 * ((2 * N_LAT - 2 - lat) // N_LAT)
    pl.semaphore_wait(barrier, neighbours)

    def row_copy(side, ch):
        return pltpu.make_async_remote_copy(
            src_ref=rsend.at[side, ch], dst_ref=rrecv.at[side, ch],
            send_sem=rs_sem.at[side, ch], recv_sem=rr_sem.at[side, ch],
            device_id=at(2 * side - 1, 0), device_id_type=MESH,
        )

    def edge_copy(e):
        dlat, dlon = EDGES[e]
        place = EDGES.index((-dlat, -dlon))
        return pltpu.make_async_remote_copy(
            src_ref=esend, dst_ref=erecv.at[place],
            send_sem=es_sem.at[e], recv_sem=er_sem.at[place],
            device_id=at(dlat, dlon), device_id_type=MESH,
        )

    @pl.when(lat > 0)
    def _():
        edge_copy(2).start()
        edge_copy(3).start()

    @pl.when(lat < N_LAT - 1)
    def _():
        edge_copy(4).start()
        edge_copy(5).start()

    edge_copy(0).start()
    edge_copy(1).start()
    for ch in range(NCH):

        @pl.when(lat > 0)
        def _():
            row_copy(0, ch).start()

        @pl.when(lat < N_LAT - 1)
        def _():
            row_copy(1, ch).start()

    @pl.when(lat == 0)
    def _():
        rrecv[1] = jnp.zeros(rrecv.shape[1:], BF16)
        erecv[2] = jnp.zeros(erecv.shape[1:], BF16)
        erecv[3] = jnp.zeros(erecv.shape[1:], BF16)

    @pl.when(lat == N_LAT - 1)
    def _():
        rrecv[0] = jnp.zeros(rrecv.shape[1:], BF16)
        erecv[4] = jnp.zeros(erecv.shape[1:], BF16)
        erecv[5] = jnp.zeros(erecv.shape[1:], BF16)

    def block(n, slot):
        if isinstance(n, int) and n == OZ:
            return oz.at[slot]
        return qb.at[slot, pl.ds(n * CH, CH)]

    def send(n, flow, source, slot, dlon):
        return pltpu.make_async_remote_copy(
            src_ref=block(n, source), dst_ref=block(n, slot),
            send_sem=qs_sem.at[n, flow], recv_sem=qr_sem.at[n, slot],
            device_id=at(0, dlon), device_id_type=MESH,
        )

    def first_hops(n, act):
        @pl.when(core == 0)
        def _():
            act(send(n, 0, 0, 2, 2))
            act(send(n, 1, 0, 1, 1))

        @pl.when(core == 1)
        def _():
            act(send(n, 0, 0, 3, 3))

        @pl.when(quarter == 1)
        def _():
            act(send(n, 1, 0, 2, 2))

    def arrived(n, slot):
        send(n, 0, 0, slot, 1).wait_recv()

    def forward(n):
        @pl.when(core == 0)
        def _():
            arrived(n, 3)

        @pl.when(quarter == 2)
        def _():
            send(n, 2, 3, 2, -1).start()

        arrived(n, 2)

        @pl.when(core == 0)
        def _():
            send(n, 3, 2, 3, 1).start()

        @pl.when(core == 1)
        def _():
            send(n, 3, 2, 1, -1).start()

    def complete(n):
        arrived(n, 1)

        @pl.when(core == 1)
        def _():
            arrived(n, 3)

    def drain(n):
        first_hops(n, lambda copy: copy.wait_send())

        @pl.when(quarter == 2)
        def _():
            send(n, 2, 3, 2, -1).wait_send()

        @pl.when(core == 0)
        def _():
            send(n, 3, 2, 3, 1).wait_send()

        @pl.when(core == 1)
        def _():
            send(n, 3, 2, 1, -1).wait_send()

    loads[1].wait()
    for j in range(ROWS):
        oz[0, j] = st[pl.ds(7 * FIELD + j, LEV, stride=ROWS), :].astype(BF16)
    first_hops(OZ, lambda copy: copy.start())
    loads[2].wait()
    sf[...] = sfb[...].astype(F32)
    loads[3].wait()
    listed = lit[...]
    row_id = lax.broadcasted_iota(jnp.int32, (ROWS, COLS), 0)
    col_id = lax.broadcasted_iota(jnp.int32, (COLS, COLS), 0)
    in_row, in_col = [], []
    for r in range(ROWS):
        entry = listed[r : r + 1]
        in_row.append(jnp.where(jnp.broadcast_to(entry >> 7, (ROWS, COLS)) == row_id, 1.0, 0.0))
        in_col.append(jnp.where(jnp.broadcast_to(entry & 127, (COLS, COLS)) == col_id, 1.0, 0.0))
    mask[...] = nt(jnp.concatenate(in_row, 1).astype(BF16), jnp.concatenate(in_col, 1).astype(BF16))
    loads[4].wait()
    eye_c = eye(COLS)

    def static_rows(j, carry):
        tracers = st[pl.ds(DYN * ROWS + j, 8 * LEV - DYN, stride=ROWS), :]
        ground = sf[pl.ds(j, 76, stride=ROWS), :]
        x = jnp.concatenate([tracers, ground], axis=0).astype(BF16)
        xt = nt(eye_c, x).astype(BF16)
        spot = pl.ds(pl.multiple_of(j * COLS, COLS), COLS)
        acc[spot, :] = jnp.dot(xt, w1[DYN:NIN], preferred_element_type=F32)
        return carry

    lax.fori_loop(0, ROWS, static_rows, 0)
    loads[5].wait()

    @pl.when(lat > 0)
    def _():
        edge_copy(5).wait_recv()
        edge_copy(4).wait_recv()

    @pl.when(lat < N_LAT - 1)
    def _():
        edge_copy(3).wait_recv()
        edge_copy(2).wait_recv()

    edge_copy(1).wait_recv()
    edge_copy(0).wait_recv()
    edge_shape = (3 * GROUPS * ROWS, COLS)
    west_half = lax.broadcasted_iota(jnp.int32, edge_shape, 1) % 8 < 4
    north_half = lax.broadcasted_iota(jnp.int32, edge_shape, 0) % 8 < 4
    edge = [erecv[e].astype(F32) for e in range(6)]
    ca[...] = jnp.where(west_half, edge[0], edge[1])
    cb[...] = jnp.where(north_half, jnp.where(west_half, edge[4], edge[5]), jnp.where(west_half, edge[2], edge[3]))

    shape = (LC, ROWS, COLS)
    lane = lax.broadcasted_iota(jnp.int32, shape, 2)
    sub = lax.broadcasted_iota(jnp.int32, shape, 1)
    first_lane, last_lane, first_sub, last_sub = lane == 0, lane == COLS - 1, sub == 0, sub == ROWS - 1
    row_a = lat * ROWS + sub
    row_b = lat * ROWS + jnp.where(sub < 4, sub + ROWS, sub - ROWS)
    open_a = row_a < N_LAT * ROWS - 1
    open_b = jnp.logical_and(row_b >= 0, row_b < N_LAT * ROWS - 1)

    def swap(edge_mask, x, y):
        return jnp.where(edge_mask, y, x), jnp.where(edge_mask, x, y)

    def east(x, h):
        return swap(last_lane, pltpu.roll(x, COLS - 1, 2), pltpu.roll(h, COLS - 1, 2))

    def west(x, h):
        return swap(first_lane, pltpu.roll(x, 1, 2), pltpu.roll(h, 1, 2))

    def north(x, h):
        return swap(last_sub, pltpu.roll(x, ROWS - 1, 1), pltpu.roll(h, ROWS - 1, 1))

    def south(x, h):
        return swap(first_sub, pltpu.roll(x, 1, 1), pltpu.roll(h, 1, 1))

    def acoustic(ch, carry):
        @pl.when(lat > 0)
        def _():
            row_copy(1, ch).wait_recv()

        @pl.when(lat < N_LAT - 1)
        def _():
            row_copy(0, ch).wait_recv()

        half = lax.broadcasted_iota(jnp.int32, (HC, ROWS, COLS), 1) < 4
        quads = []
        for f in range(3):
            spot = pl.ds(pl.multiple_of(f * FIELD + ch * LC * ROWS, ROWS), LC * ROWS)
            a = st[spot, :].reshape(shape)
            rows = slice(f * HC * ROWS, (f + 1) * HC * ROWS)
            nn = rrecv[0, ch, rows].astype(F32).reshape(HC, ROWS, COLS)
            ss = rrecv[1, ch, rows].astype(F32).reshape(HC, ROWS, COLS)
            b = jnp.concatenate(
                [jnp.where(half, nn, pltpu.roll(ss, 4, 1)), jnp.where(half, pltpu.roll(nn, 4, 1), ss)], axis=0
            )
            sides = []
            for source in (ca, cb):
                pieces = []
                for g in range(LC // PER):
                    at_row = pl.multiple_of((f * GROUPS + ch * (LC // PER) + g) * ROWS, ROWS)
                    group = source[pl.ds(at_row, ROWS), :]
                    for kk in range(PER):
                        pieces.append(pltpu.roll(group, (COLS - 4 - 8 * kk) % COLS, 1).reshape(1, ROWS, COLS))
                sides.append(jnp.concatenate(pieces, axis=0))
            quads.append((a, b, sides[0], sides[1]))
        za, zb, zc, zd = quads[0]
        ma, mb, mc, md = quads[1]
        pa, pb, pc, pd = quads[2]
        ma, mc = jnp.where(open_a, ma, 0.0), jnp.where(open_a, mc, 0.0)
        mb, md = jnp.where(open_b, mb, 0.0), jnp.where(open_b, md, 0.0)
        zwa, zwc = west(za, zc)
        zwb, zwd = west(zb, zd)
        msa, msb = south(ma, mb)
        msc, msd = south(mc, md)
        da = COURANT * (za - zwa + ma - msa)
        db = COURANT * (zb - zwb + mb - msb)
        dc = COURANT * (zc - zwc + mc - msc)
        dd = COURANT * (zd - zwd + md - msd)
        sa, sb, sc, sd = pa, pb, pc, pd
        square = COURANT * COURANT
        for step in range(1, 5):
            ea, ec = east(sa, sc)
            wa, wc = west(sa, sc)
            na, nb = north(sa, sb)
            ga, gb = jnp.where(open_a, na - sa, 0.0), jnp.where(open_b, nb - sb, 0.0)
            gsa, gsb = south(ga, gb)
            new_pa = pa - da + square * (ea + wa - 2.0 * sa + ga - gsa)
            if step < 4:
                eb, ed = east(sb, sd)
                wb, wd = west(sb, sd)
                nc, nd = north(sc, sd)
                gc, gd = jnp.where(open_a, nc - sc, 0.0), jnp.where(open_b, nd - sd, 0.0)
                gsc, gsd = south(gc, gd)
                pb = pb - db + square * (eb + wb - 2.0 * sb + gb - gsb)
                pc = pc - dc + square * (ec + wc - 2.0 * sc + gc - gsc)
                if step < 3:
                    pd = pd - dd + square * (ed + wd - 2.0 * sd + gd - gsd)
                pa = new_pa
                sa, sb, sc, sd = sa + pa, sb + pb, sc + pc, sd + pd
            else:
                pa = new_pa
        za = za - COURANT * (ea - sa)
        zc = zc - COURANT * (ec - sc)
        ma = jnp.where(open_a, ma - COURANT * ga, 0.0)
        z_west, _ = west(za, zc)
        share = (0.5 + 0.45 * jnp.tanh(za)).reshape(LC * ROWS, COLS)
        share_west = (0.5 + 0.45 * jnp.tanh(z_west)).reshape(LC * ROWS, COLS)
        for f, value in enumerate((za, ma, pa)):
            spot = pl.ds(pl.multiple_of(f * FIELD + ch * LC * ROWS, ROWS), LC * ROWS)
            st[spot, :] = value.reshape(LC * ROWS, COLS)
        out[pl.ds(pl.multiple_of(2 * FIELD + ch * LC * ROWS, ROWS), LC * ROWS), :] = pa.reshape(LC * ROWS, COLS)
        for f in range(4):
            spot = pl.ds(pl.multiple_of(f * FIELD + ch * LC * ROWS, ROWS), LC * ROWS)
            fr[spot, :] = share
            fw[spot, :] = share_west
        return carry

    lax.fori_loop(0, NCH, acoustic, 0)

    for load in loads[6:]:
        load.wait()

    def network(n, carry):
        xs = []
        for r in range(CH):
            x = st[pl.ds(n * CH + r, DYN, stride=ROWS), :].astype(BF16)
            xs.append(nt(eye_c, x).astype(BF16))
        xt = jnp.concatenate(xs, axis=0)
        spot = pl.ds(pl.multiple_of(n * CH * COLS, COLS), CH * COLS)
        h = leaky(acc[spot, :] + jnp.dot(xt, w1[0:DYN], preferred_element_type=F32))
        for w in (w2, w3, w4):
            h = leaky(jnp.dot(h, w[...], preferred_element_type=F32))
        y = nt(w5t[...], h)
        for r in range(CH):
            j = n * CH + r
            t = jnp.where(jnp.broadcast_to(mask[pl.ds(j, 1), :], (NOUT, COLS)) > 0.5, y[:, r * COLS : (r + 1) * COLS], 0.0)
            out[pl.ds(j, 2 * LEV, stride=ROWS), :] = st[pl.ds(j, 2 * LEV, stride=ROWS), :] + STEP * t[0 : 2 * LEV]
            q = st[pl.ds(3 * FIELD + j, 4 * LEV, stride=ROWS), :] + STEP * t[2 * LEV : 6 * LEV]
            qb[0, j] = q.astype(BF16)
            fl[pl.ds(j, 8, stride=ROWS), :] = t[6 * LEV :]
        first_hops(n, lambda copy: copy.start())
        return carry

    lax.fori_loop(0, NB, network, 0)
    flux[...] = fl[...].astype(BF16)

    def advect(j, ref, count, base):
        offset = off[j]
        tiles, cells = offset >> 7, offset & 127
        tile_shape = (count, COLS)
        where = lax.broadcasted_iota(jnp.int32, tile_shape, 1)
        parts = [ref[slot, j].astype(F32) for slot in range(4)]

        def pick(cut):
            d = tiles + jnp.where(where >= cut, 1, 0)
            return jnp.where(d == 0, parts[0], jnp.where(d == 1, parts[1], jnp.where(d == 2, parts[2], parts[3])))

        near = pltpu.roll(pick(COLS - cells), cells, 1)
        far = pltpu.roll(pick(COLS - 1 - cells), (cells + 1) & 127, 1)
        spot = pl.ds(j, count, stride=ROWS)
        value = (1.0 - fr[spot, :]) * near + fw[spot, :] * far
        out[pl.ds(base * FIELD + j, count, stride=ROWS), :] = value

    forward(OZ)

    def tracer_block(n, carry):
        forward(n)
        complete(n)
        for r in range(CH):
            advect(n * CH + r, qb, 4 * LEV, 3)
        return carry

    complete(OZ)

    def ozone_row(j, carry):
        advect(j, oz, LEV, 7)
        return carry

    lax.fori_loop(0, ROWS, ozone_row, 0)
    lax.fori_loop(0, NB, tracer_block, 0)

    @pl.when(lat > 0)
    def _():
        edge_copy(2).wait_send()
        edge_copy(3).wait_send()

    @pl.when(lat < N_LAT - 1)
    def _():
        edge_copy(4).wait_send()
        edge_copy(5).wait_send()

    edge_copy(0).wait_send()
    edge_copy(1).wait_send()
    for ch in range(NCH):

        @pl.when(lat > 0)
        def _():
            row_copy(0, ch).wait_send()

        @pl.when(lat < N_LAT - 1)
        def _():
            row_copy(1, ch).wait_send()

    drain(OZ)

    def drain_block(n, carry):
        drain(n)
        return carry

    lax.fori_loop(0, NB, drain_block, 0)


def on_device(state, surface, layer_one, layer_two, layer_three, layer_four, layer_five, lit_columns, row_offset):
    fields = state.shape[0]
    any_spec = pl.BlockSpec(memory_space=pl.ANY)
    vmem_spec = pl.BlockSpec(memory_space=pltpu.VMEM)
    dma = pltpu.SemaphoreType.DMA
    new_state, surface_flux = pl.pallas_call(
        kernel,
        out_shape=(
            jax.ShapeDtypeStruct((fields * FIELD, COLS), F32),
            jax.ShapeDtypeStruct((8 * ROWS, COLS), BF16),
        ),
        in_specs=[any_spec] * 8 + [pl.BlockSpec(memory_space=pltpu.SMEM)],
        out_specs=(vmem_spec, vmem_spec),
        scratch_shapes=[
            pltpu.VMEM((fields * FIELD, COLS), F32),
            pltpu.VMEM((76 * ROWS, COLS), BF16),
            pltpu.VMEM((76 * ROWS, COLS), F32),
            pltpu.VMEM((NIN, H1), BF16),
            pltpu.VMEM((H1, H2), BF16),
            pltpu.VMEM((H2, H3), BF16),
            pltpu.VMEM((H3, H4), BF16),
            pltpu.VMEM((NOUT, H4), BF16),
            pltpu.VMEM((ROWS, COLS), jnp.int32),
            pltpu.VMEM((ROWS * COLS, H1), F32),
            pltpu.VMEM((ROWS, COLS), F32),
            pltpu.VMEM((4 * FIELD, COLS), F32),
            pltpu.VMEM((4 * FIELD, COLS), F32),
            pltpu.VMEM((8 * ROWS, COLS), F32),
            pltpu.VMEM((2, NCH, 3 * HC * ROWS, COLS), BF16),
            pltpu.VMEM((2, NCH, 3 * HC * ROWS, COLS), BF16),
            pltpu.VMEM((3 * GROUPS * ROWS, COLS), BF16),
            pltpu.VMEM((6, 3 * GROUPS * ROWS, COLS), BF16),
            pltpu.VMEM((3 * GROUPS * ROWS, COLS), F32),
            pltpu.VMEM((3 * GROUPS * ROWS, COLS), F32),
            pltpu.VMEM((4, ROWS, LEV, COLS), BF16),
            pltpu.VMEM((4, ROWS, 4 * LEV, COLS), BF16),
            dma((9,)),
            dma((2, NCH)),
            dma((2, NCH)),
            dma((6,)),
            dma((6,)),
            dma((NB + 1, 4)),
            dma((NB + 1, 4)),
        ],
        compiler_params=pltpu.CompilerParams(
            collective_id=0, has_side_effects=True, vmem_limit_bytes=56 * 1024 * 1024
        ),
    )(
        state.reshape(fields * FIELD, COLS),
        surface.reshape(76 * ROWS, COLS),
        layer_one, layer_two, layer_three, layer_four, layer_five.T,
        lit_columns.reshape(ROWS, COLS),
        row_offset,
    )
    return new_state.reshape(fields, LEV, ROWS, COLS), surface_flux.reshape(8, ROWS, COLS)


def solution(mesh):
    in_specs = (
        P(None, None, "lat", "lon"), P(None, "lat", "lon"), P(), P(), P(), P(), P(), P("lat", "lon", None), P("lat"),
    )
    out_specs = (P(None, None, "lat", "lon"), P(None, "lat", "lon"))
    return jax.shard_map(on_device, mesh=mesh, in_specs=in_specs, out_specs=out_specs, check_vma=False)
```

```python
import jax
import jax.numpy as jnp
from jax import lax
from jax.experimental import pallas as pl
from jax.experimental.pallas import tpu as pltpu
from jax.sharding import PartitionSpec as P

MESH = pl.DeviceIdType.MESH
F32, BF16 = jnp.float32, jnp.bfloat16

N_LAT, N_LON = 8, 16
LEV = 60
ROWS, COLS = 8, 128
FIELD = LEV * ROWS
COURANT = 0.6
STEP = 0.5
SLOPE = 0.15
DYN = 192
NIN, NOUT = 556, 368
H1, H2, H3, H4 = 768, 640, 512, 640

LC = 20
NCH = LEV // LC
HC = LC // 2
PER = 10
GROUPS = LEV // PER
CH = 2
NB = ROWS // CH
OZ = NB

EDGES = ((0, -1), (0, 1), (-1, -1), (-1, 1), (1, -1), (1, 1))


def nt(a, b):
    return lax.dot_general(a, b, (((1,), (1,)), ((), ())), preferred_element_type=F32)


def eye(n):
    return (lax.broadcasted_iota(jnp.int32, (n, n), 0) == lax.broadcasted_iota(jnp.int32, (n, n), 1)).astype(F32).astype(BF16)


def leaky(z):
    return jnp.maximum(z, SLOPE * z).astype(BF16)


def kernel(
    state, surface, w1h, w2h, w3h, w4h, w5h, lith, off,
    out, flux,
    st, sfb, sf, w1, w2, w3, w4, w5t, lit, acc, mask, fr, fw, fl,
    rsend, rrecv, esend, erecv, ca, cb, oz, qb,
    load_sem, rs_sem, rr_sem, es_sem, er_sem, qs_sem, qr_sem,
):
    lat, lon = lax.axis_index("lat"), lax.axis_index("lon")
    core, quarter = lax.rem(lon, 2), lax.rem(lon, 4)

    def at(dlat, dlon):
        return (lat + dlat, lax.rem(lon + dlon + N_LON, N_LON))

    loads = [
        pltpu.make_async_copy(state.at[0 : 3 * FIELD], st.at[0 : 3 * FIELD], load_sem.at[0]),
        pltpu.make_async_copy(state.at[3 * FIELD : 8 * FIELD], st.at[3 * FIELD : 8 * FIELD], load_sem.at[1]),
        pltpu.make_async_copy(surface, sfb, load_sem.at[2]),
        pltpu.make_async_copy(lith, lit, load_sem.at[3]),
        pltpu.make_async_copy(w1h, w1, load_sem.at[4]),
        pltpu.make_async_copy(w5h, w5t, load_sem.at[5]),
        pltpu.make_async_copy(w2h, w2, load_sem.at[6]),
        pltpu.make_async_copy(w3h, w3, load_sem.at[7]),
        pltpu.make_async_copy(w4h, w4, load_sem.at[8]),
    ]
    for load in loads:
        load.start()

    barrier = pltpu.get_barrier_semaphore()

    def greet(dlat, dlon):
        pl.semaphore_signal(barrier, inc=1, device_id=at(dlat, dlon), device_id_type=MESH)

    for dlon in (-3, -2, -1, 1, 2, 3):
        greet(0, dlon)

    @pl.when(lat > 0)
    def _():
        for dlon in (-1, 0, 1):
            greet(-1, dlon)

    @pl.when(lat < N_LAT - 1)
    def _():
        for dlon in (-1, 0, 1):
            greet(1, dlon)

    loads[0].wait()
    sub3 = lax.broadcasted_iota(jnp.int32, (HC, ROWS, COLS), 1) < 4
    for ch in range(NCH):
        for f in range(3):
            x = st[f * FIELD + ch * LC * ROWS : f * FIELD + (ch + 1) * LC * ROWS].reshape(LC, ROWS, COLS)
            low, high = x[:HC], x[HC:]
            to_south = jnp.where(sub3, low, pltpu.roll(high, 4, 1))
            to_north = jnp.where(sub3, pltpu.roll(low, 4, 1), high)
            spot = slice(f * HC * ROWS, (f + 1) * HC * ROWS)
            rsend[0, ch, spot] = to_south.reshape(HC * ROWS, COLS).astype(BF16)
            rsend[1, ch, spot] = to_north.reshape(HC * ROWS, COLS).astype(BF16)
    lane2 = lax.broadcasted_iota(jnp.int32, (ROWS, COLS), 1)
    packed = []
    for f in range(3):
        for g in range(GROUPS):
            total = jnp.zeros((ROWS, COLS), F32)
            for kk in range(PER):
                row = (f * LEV + g * PER + kk) * ROWS
                total = jnp.where(lane2 // 8 == kk, pltpu.roll(st[row : row + ROWS], 4 + 8 * kk, 1), total)
            packed.append(total)
    esend[...] = jnp.concatenate(packed, axis=0).astype(BF16)

    neighbours = 6 + 3 * ((lat + N_LAT - 1) // N_LAT) + 3 * ((2 * N_LAT - 2 - lat) // N_LAT)
    pl.semaphore_wait(barrier, neighbours)

    def row_copy(side, ch):
        return pltpu.make_async_remote_copy(
            src_ref=rsend.at[side, ch], dst_ref=rrecv.at[side, ch],
            send_sem=rs_sem.at[side, ch], recv_sem=rr_sem.at[side, ch],
            device_id=at(2 * side - 1, 0), device_id_type=MESH,
        )

    def edge_copy(e):
        dlat, dlon = EDGES[e]
        place = EDGES.index((-dlat, -dlon))
        return pltpu.make_async_remote_copy(
            src_ref=esend, dst_ref=erecv.at[place],
            send_sem=es_sem.at[e], recv_sem=er_sem.at[place],
            device_id=at(dlat, dlon), device_id_type=MESH,
        )

    @pl.when(lat > 0)
    def _():
        edge_copy(2).start()
        edge_copy(3).start()

    @pl.when(lat < N_LAT - 1)
    def _():
        edge_copy(4).start()
        edge_copy(5).start()

    edge_copy(0).start()
    edge_copy(1).start()
    for ch in range(NCH):

        @pl.when(lat > 0)
        def _():
            row_copy(0, ch).start()

        @pl.when(lat < N_LAT - 1)
        def _():
            row_copy(1, ch).start()

    @pl.when(lat == 0)
    def _():
        rrecv[1] = jnp.zeros(rrecv.shape[1:], BF16)
        erecv[2] = jnp.zeros(erecv.shape[1:], BF16)
        erecv[3] = jnp.zeros(erecv.shape[1:], BF16)

    @pl.when(lat == N_LAT - 1)
    def _():
        rrecv[0] = jnp.zeros(rrecv.shape[1:], BF16)
        erecv[4] = jnp.zeros(erecv.shape[1:], BF16)
        erecv[5] = jnp.zeros(erecv.shape[1:], BF16)

    def block(n, slot):
        if isinstance(n, int) and n == OZ:
            return oz.at[slot]
        return qb.at[slot, pl.ds(n * CH, CH)]

    def send(n, flow, source, slot, dlon):
        return pltpu.make_async_remote_copy(
            src_ref=block(n, source), dst_ref=block(n, slot),
            send_sem=qs_sem.at[n, flow], recv_sem=qr_sem.at[n, slot],
            device_id=at(0, dlon), device_id_type=MESH,
        )

    def first_hops(n, act):
        @pl.when(core == 0)
        def _():
            act(send(n, 0, 0, 2, 2))
            act(send(n, 1, 0, 1, 1))

        @pl.when(core == 1)
        def _():
            act(send(n, 0, 0, 3, 3))

        @pl.when(quarter == 1)
        def _():
            act(send(n, 1, 0, 2, 2))

    def arrived(n, slot):
        send(n, 0, 0, slot, 1).wait_recv()

    def forward(n):
        @pl.when(core == 0)
        def _():
            arrived(n, 3)

        @pl.when(quarter == 2)
        def _():
            send(n, 2, 3, 2, -1).start()

        arrived(n, 2)

        @pl.when(core == 0)
        def _():
            send(n, 3, 2, 3, 1).start()

        @pl.when(core == 1)
        def _():
            send(n, 3, 2, 1, -1).start()

    def complete(n):
        arrived(n, 1)

        @pl.when(core == 1)
        def _():
            arrived(n, 3)

    def drain(n):
        first_hops(n, lambda copy: copy.wait_send())

        @pl.when(quarter == 2)
        def _():
            send(n, 2, 3, 2, -1).wait_send()

        @pl.when(core == 0)
        def _():
            send(n, 3, 2, 3, 1).wait_send()

        @pl.when(core == 1)
        def _():
            send(n, 3, 2, 1, -1).wait_send()

    loads[1].wait()
    for j in range(ROWS):
        oz[0, j] = st[pl.ds(7 * FIELD + j, LEV, stride=ROWS), :].astype(BF16)
    first_hops(OZ, lambda copy: copy.start())
    loads[2].wait()
    sf[...] = sfb[...].astype(F32)
    loads[3].wait()
    listed = lit[...]
    row_id = lax.broadcasted_iota(jnp.int32, (ROWS, COLS), 0)
    col_id = lax.broadcasted_iota(jnp.int32, (COLS, COLS), 0)
    in_row, in_col = [], []
    for r in range(ROWS):
        entry = listed[r : r + 1]
        in_row.append(jnp.where(jnp.broadcast_to(entry >> 7, (ROWS, COLS)) == row_id, 1.0, 0.0))
        in_col.append(jnp.where(jnp.broadcast_to(entry & 127, (COLS, COLS)) == col_id, 1.0, 0.0))
    mask[...] = nt(jnp.concatenate(in_row, 1).astype(BF16), jnp.concatenate(in_col, 1).astype(BF16))
    loads[4].wait()
    eye_c = eye(COLS)

    def static_rows(j, carry):
        tracers = st[pl.ds(DYN * ROWS + j, 8 * LEV - DYN, stride=ROWS), :]
        ground = sf[pl.ds(j, 76, stride=ROWS), :]
        x = jnp.concatenate([tracers, ground], axis=0).astype(BF16)
        xt = nt(eye_c, x).astype(BF16)
        spot = pl.ds(pl.multiple_of(j * COLS, COLS), COLS)
        acc[spot, :] = jnp.dot(xt, w1[DYN:NIN], preferred_element_type=F32)
        return carry

    lax.fori_loop(0, ROWS, static_rows, 0)
    loads[5].wait()

    @pl.when(lat > 0)
    def _():
        edge_copy(5).wait_recv()
        edge_copy(4).wait_recv()

    @pl.when(lat < N_LAT - 1)
    def _():
        edge_copy(3).wait_recv()
        edge_copy(2).wait_recv()

    edge_copy(1).wait_recv()
    edge_copy(0).wait_recv()
    edge_shape = (3 * GROUPS * ROWS, COLS)
    west_half = lax.broadcasted_iota(jnp.int32, edge_shape, 1) % 8 < 4
    north_half = lax.broadcasted_iota(jnp.int32, edge_shape, 0) % 8 < 4
    edge = [erecv[e].astype(F32) for e in range(6)]
    ca[...] = jnp.where(west_half, edge[0], edge[1])
    cb[...] = jnp.where(north_half, jnp.where(west_half, edge[4], edge[5]), jnp.where(west_half, edge[2], edge[3]))

    shape = (LC, ROWS, COLS)
    lane = lax.broadcasted_iota(jnp.int32, shape, 2)
    sub = lax.broadcasted_iota(jnp.int32, shape, 1)
    first_lane, last_lane, first_sub, last_sub = lane == 0, lane == COLS - 1, sub == 0, sub == ROWS - 1
    row_a = lat * ROWS + sub
    row_b = lat * ROWS + jnp.where(sub < 4, sub + ROWS, sub - ROWS)
    open_a = row_a < N_LAT * ROWS - 1
    open_b = jnp.logical_and(row_b >= 0, row_b < N_LAT * ROWS - 1)

    def swap(edge_mask, x, y):
        return jnp.where(edge_mask, y, x), jnp.where(edge_mask, x, y)

    def east(x, h):
        return swap(last_lane, pltpu.roll(x, COLS - 1, 2), pltpu.roll(h, COLS - 1, 2))

    def west(x, h):
        return swap(first_lane, pltpu.roll(x, 1, 2), pltpu.roll(h, 1, 2))

    def north(x, h):
        return swap(last_sub, pltpu.roll(x, ROWS - 1, 1), pltpu.roll(h, ROWS - 1, 1))

    def south(x, h):
        return swap(first_sub, pltpu.roll(x, 1, 1), pltpu.roll(h, 1, 1))

    def acoustic(ch, carry):
        @pl.when(lat > 0)
        def _():
            row_copy(1, ch).wait_recv()

        @pl.when(lat < N_LAT - 1)
        def _():
            row_copy(0, ch).wait_recv()

        half = lax.broadcasted_iota(jnp.int32, (HC, ROWS, COLS), 1) < 4
        quads = []
        for f in range(3):
            spot = pl.ds(pl.multiple_of(f * FIELD + ch * LC * ROWS, ROWS), LC * ROWS)
            a = st[spot, :].reshape(shape)
            rows = slice(f * HC * ROWS, (f + 1) * HC * ROWS)
            nn = rrecv[0, ch, rows].astype(F32).reshape(HC, ROWS, COLS)
            ss = rrecv[1, ch, rows].astype(F32).reshape(HC, ROWS, COLS)
            b = jnp.concatenate(
                [jnp.where(half, nn, pltpu.roll(ss, 4, 1)), jnp.where(half, pltpu.roll(nn, 4, 1), ss)], axis=0
            )
            sides = []
            for source in (ca, cb):
                pieces = []
                for g in range(LC // PER):
                    at_row = pl.multiple_of((f * GROUPS + ch * (LC // PER) + g) * ROWS, ROWS)
                    group = source[pl.ds(at_row, ROWS), :]
                    for kk in range(PER):
                        pieces.append(pltpu.roll(group, (COLS - 4 - 8 * kk) % COLS, 1).reshape(1, ROWS, COLS))
                sides.append(jnp.concatenate(pieces, axis=0))
            quads.append((a, b, sides[0], sides[1]))
        za, zb, zc, zd = quads[0]
        ma, mb, mc, md = quads[1]
        pa, pb, pc, pd = quads[2]
        ma, mc = jnp.where(open_a, ma, 0.0), jnp.where(open_a, mc, 0.0)
        mb, md = jnp.where(open_b, mb, 0.0), jnp.where(open_b, md, 0.0)
        zwa, zwc = west(za, zc)
        zwb, zwd = west(zb, zd)
        msa, msb = south(ma, mb)
        msc, msd = south(mc, md)
        da = COURANT * (za - zwa + ma - msa)
        db = COURANT * (zb - zwb + mb - msb)
        dc = COURANT * (zc - zwc + mc - msc)
        dd = COURANT * (zd - zwd + md - msd)
        sa, sb, sc, sd = pa, pb, pc, pd
        square = COURANT * COURANT
        for step in range(1, 5):
            ea, ec = east(sa, sc)
            wa, wc = west(sa, sc)
            na, nb = north(sa, sb)
            ga, gb = jnp.where(open_a, na - sa, 0.0), jnp.where(open_b, nb - sb, 0.0)
            gsa, gsb = south(ga, gb)
            new_pa = pa - da + square * (ea + wa - 2.0 * sa + ga - gsa)
            if step < 4:
                eb, ed = east(sb, sd)
                wb, wd = west(sb, sd)
                nc, nd = north(sc, sd)
                gc, gd = jnp.where(open_a, nc - sc, 0.0), jnp.where(open_b, nd - sd, 0.0)
                gsc, gsd = south(gc, gd)
                pb = pb - db + square * (eb + wb - 2.0 * sb + gb - gsb)
                pc = pc - dc + square * (ec + wc - 2.0 * sc + gc - gsc)
                if step < 3:
                    pd = pd - dd + square * (ed + wd - 2.0 * sd + gd - gsd)
                pa = new_pa
                sa, sb, sc, sd = sa + pa, sb + pb, sc + pc, sd + pd
            else:
                pa = new_pa
        za = za - COURANT * (ea - sa)
        zc = zc - COURANT * (ec - sc)
        ma = jnp.where(open_a, ma - COURANT * ga, 0.0)
        z_west, _ = west(za, zc)
        share = (0.5 + 0.45 * jnp.tanh(za)).reshape(LC * ROWS, COLS)
        share_west = (0.5 + 0.45 * jnp.tanh(z_west)).reshape(LC * ROWS, COLS)
        for f, value in enumerate((za, ma, pa)):
            spot = pl.ds(pl.multiple_of(f * FIELD + ch * LC * ROWS, ROWS), LC * ROWS)
            st[spot, :] = value.reshape(LC * ROWS, COLS)
        out[pl.ds(pl.multiple_of(2 * FIELD + ch * LC * ROWS, ROWS), LC * ROWS), :] = pa.reshape(LC * ROWS, COLS)
        for f in range(4):
            spot = pl.ds(pl.multiple_of(f * FIELD + ch * LC * ROWS, ROWS), LC * ROWS)
            fr[spot, :] = share
            fw[spot, :] = share_west
        return carry

    lax.fori_loop(0, NCH, acoustic, 0)

    for load in loads[6:]:
        load.wait()

    def network(n, carry):
        xs = []
        for r in range(CH):
            x = st[pl.ds(n * CH + r, DYN, stride=ROWS), :].astype(BF16)
            xs.append(nt(eye_c, x).astype(BF16))
        xt = jnp.concatenate(xs, axis=0)
        spot = pl.ds(pl.multiple_of(n * CH * COLS, COLS), CH * COLS)
        h = leaky(acc[spot, :] + jnp.dot(xt, w1[0:DYN], preferred_element_type=F32))
        for w in (w2, w3, w4):
            h = leaky(jnp.dot(h, w[...], preferred_element_type=F32))
        y = nt(w5t[...], h)
        for r in range(CH):
            j = n * CH + r
            t = jnp.where(jnp.broadcast_to(mask[pl.ds(j, 1), :], (NOUT, COLS)) > 0.5, y[:, r * COLS : (r + 1) * COLS], 0.0)
            out[pl.ds(j, 2 * LEV, stride=ROWS), :] = st[pl.ds(j, 2 * LEV, stride=ROWS), :] + STEP * t[0 : 2 * LEV]
            q = st[pl.ds(3 * FIELD + j, 4 * LEV, stride=ROWS), :] + STEP * t[2 * LEV : 6 * LEV]
            qb[0, j] = q.astype(BF16)
            fl[pl.ds(j, 8, stride=ROWS), :] = t[6 * LEV :]
        first_hops(n, lambda copy: copy.start())
        return carry

    lax.fori_loop(0, NB, network, 0)
    flux[...] = fl[...].astype(BF16)

    def advect(j, ref, count, base):
        offset = off[j]
        tiles, cells = offset >> 7, offset & 127
        tile_shape = (count, COLS)
        where = lax.broadcasted_iota(jnp.int32, tile_shape, 1)
        parts = [ref[slot, j].astype(F32) for slot in range(4)]

        def pick(cut):
            d = tiles + jnp.where(where >= cut, 1, 0)
            return jnp.where(d == 0, parts[0], jnp.where(d == 1, parts[1], jnp.where(d == 2, parts[2], parts[3])))

        near = pltpu.roll(pick(COLS - cells), cells, 1)
        far = pltpu.roll(pick(COLS - 1 - cells), (cells + 1) & 127, 1)
        spot = pl.ds(j, count, stride=ROWS)
        value = (1.0 - fr[spot, :]) * near + fw[spot, :] * far
        out[pl.ds(base * FIELD + j, count, stride=ROWS), :] = value

    forward(OZ)

    def tracer_block(n, carry):
        forward(n)
        complete(n)
        for r in range(CH):
            advect(n * CH + r, qb, 4 * LEV, 3)
        return carry

    complete(OZ)

    def ozone_row(j, carry):
        advect(j, oz, LEV, 7)
        return carry

    lax.fori_loop(0, ROWS, ozone_row, 0)
    lax.fori_loop(0, NB, tracer_block, 0)

    @pl.when(lat > 0)
    def _():
        edge_copy(2).wait_send()
        edge_copy(3).wait_send()

    @pl.when(lat < N_LAT - 1)
    def _():
        edge_copy(4).wait_send()
        edge_copy(5).wait_send()

    edge_copy(0).wait_send()
    edge_copy(1).wait_send()
    for ch in range(NCH):

        @pl.when(lat > 0)
        def _():
            row_copy(0, ch).wait_send()

        @pl.when(lat < N_LAT - 1)
        def _():
            row_copy(1, ch).wait_send()

    drain(OZ)

    def drain_block(n, carry):
        drain(n)
        return carry

    lax.fori_loop(0, NB, drain_block, 0)


def place(state, flux, state_out, flux_out, sem):
    copies = [pltpu.make_async_copy(flux, flux_out, sem.at[4])]
    for part in range(4):
        spot = slice(part * 2 * FIELD, (part + 1) * 2 * FIELD)
        copies.append(pltpu.make_async_copy(state.at[spot], state_out.at[spot], sem.at[part]))
    for copy in copies:
        copy.start()
    for copy in copies:
        copy.wait()


def on_device(state, surface, layer_one, layer_two, layer_three, layer_four, layer_five, lit_columns, row_offset):
    fields = state.shape[0]
    any_spec = pl.BlockSpec(memory_space=pl.ANY)
    vmem_spec = pl.BlockSpec(memory_space=pltpu.VMEM)
    dma = pltpu.SemaphoreType.DMA
    new_state, surface_flux = pl.pallas_call(
        kernel,
        out_shape=(
            pltpu.VMEM((fields * FIELD, COLS), F32),
            pltpu.VMEM((8 * ROWS, COLS), BF16),
        ),
        in_specs=[any_spec] * 8 + [pl.BlockSpec(memory_space=pltpu.SMEM)],
        out_specs=(vmem_spec, vmem_spec),
        scratch_shapes=[
            pltpu.VMEM((fields * FIELD, COLS), F32),
            pltpu.VMEM((76 * ROWS, COLS), BF16),
            pltpu.VMEM((76 * ROWS, COLS), F32),
            pltpu.VMEM((NIN, H1), BF16),
            pltpu.VMEM((H1, H2), BF16),
            pltpu.VMEM((H2, H3), BF16),
            pltpu.VMEM((H3, H4), BF16),
            pltpu.VMEM((NOUT, H4), BF16),
            pltpu.VMEM((ROWS, COLS), jnp.int32),
            pltpu.VMEM((ROWS * COLS, H1), F32),
            pltpu.VMEM((ROWS, COLS), F32),
            pltpu.VMEM((4 * FIELD, COLS), F32),
            pltpu.VMEM((4 * FIELD, COLS), F32),
            pltpu.VMEM((8 * ROWS, COLS), F32),
            pltpu.VMEM((2, NCH, 3 * HC * ROWS, COLS), BF16),
            pltpu.VMEM((2, NCH, 3 * HC * ROWS, COLS), BF16),
            pltpu.VMEM((3 * GROUPS * ROWS, COLS), BF16),
            pltpu.VMEM((6, 3 * GROUPS * ROWS, COLS), BF16),
            pltpu.VMEM((3 * GROUPS * ROWS, COLS), F32),
            pltpu.VMEM((3 * GROUPS * ROWS, COLS), F32),
            pltpu.VMEM((4, ROWS, LEV, COLS), BF16),
            pltpu.VMEM((4, ROWS, 4 * LEV, COLS), BF16),
            dma((9,)),
            dma((2, NCH)),
            dma((2, NCH)),
            dma((6,)),
            dma((6,)),
            dma((NB + 1, 4)),
            dma((NB + 1, 4)),
        ],
        compiler_params=pltpu.CompilerParams(
            collective_id=0, has_side_effects=True, vmem_limit_bytes=56 * 1024 * 1024
        ),
    )(
        state.reshape(fields * FIELD, COLS),
        surface.reshape(76 * ROWS, COLS),
        layer_one, layer_two, layer_three, layer_four, layer_five.T,
        lit_columns.reshape(ROWS, COLS),
        row_offset,
    )
    new_state, surface_flux = pl.pallas_call(
        place,
        out_shape=(
            jax.ShapeDtypeStruct((fields * FIELD, COLS), F32),
            jax.ShapeDtypeStruct((8 * ROWS, COLS), BF16),
        ),
        in_specs=[vmem_spec, vmem_spec],
        out_specs=(any_spec, any_spec),
        scratch_shapes=[dma((5,))],
    )(pltpu.with_memory_space_constraint(new_state, pltpu.VMEM), pltpu.with_memory_space_constraint(surface_flux, pltpu.VMEM))
    return new_state.reshape(fields, LEV, ROWS, COLS), surface_flux.reshape(8, ROWS, COLS)


def solution(mesh):
    in_specs = (
        P(None, None, "lat", "lon"), P(None, "lat", "lon"), P(), P(), P(), P(), P(), P("lat", "lon", None), P("lat"),
    )
    out_specs = (P(None, None, "lat", "lon"), P(None, "lat", "lon"))
    return jax.shard_map(on_device, mesh=mesh, in_specs=in_specs, out_specs=out_specs, check_vma=False)
```

```python
import jax
import jax.numpy as jnp
from jax import lax
from jax.experimental import pallas as pl
from jax.experimental.pallas import tpu as pltpu
from jax.sharding import PartitionSpec as P

MESH = pl.DeviceIdType.MESH
F32, BF16 = jnp.float32, jnp.bfloat16

N_LAT, N_LON = 8, 16
LEV = 60
ROWS, COLS = 8, 128
FIELD = LEV * ROWS
COURANT = 0.6
STEP = 0.5
SLOPE = 0.15
DYN = 192
NIN, NOUT = 556, 368
H1, H2, H3, H4 = 768, 640, 512, 640

LC = 30
NCH = LEV // LC
PER = 15
GROUPS = LEV // PER
EROWS = 3 * GROUPS * ROWS
CH = 2
NB = ROWS // CH
OZ = ROWS

AROUND = ((0, -1), (0, 1), (-1, 0), (1, 0), (-1, -1), (-1, 1), (1, -1), (1, 1))
A1, B1, ZA, ZB, ZF = 0, 4, 7, 8, 9


def nt(a, b):
    return lax.dot_general(a, b, (((1,), (1,)), ((), ())), preferred_element_type=F32)


def eye(n):
    return (lax.broadcasted_iota(jnp.int32, (n, n), 0) == lax.broadcasted_iota(jnp.int32, (n, n), 1)).astype(F32).astype(BF16)


def leaky(z):
    return jnp.maximum(z, SLOPE * z).astype(BF16)


def kernel(
    state, surface, w1h, w2h, w3h, w4h, w5h, lith, off,
    out, flux,
    st, sfb, sf, w1, w2, w3, w4, w5t, lit, acc, mask, fr, fw, fl,
    own_div, rsend, rrecv, own_edge, esend, hsend, erecv, hrecv, give, oz, qb,
    load_sem, rs_sem, rr_sem, es_sem, er_sem, qs_sem, qr_sem,
):
    lat, lon = lax.axis_index("lat"), lax.axis_index("lon")
    core, quarter = lax.rem(lon, 2), lax.rem(lon, 4)

    def at(dlat, dlon):
        return (lat + dlat, lax.rem(lon + dlon + N_LON, N_LON))

    loads = [
        pltpu.make_async_copy(state.at[0 : 3 * FIELD], st.at[0 : 3 * FIELD], load_sem.at[0]),
        pltpu.make_async_copy(state.at[3 * FIELD : 8 * FIELD], st.at[3 * FIELD : 8 * FIELD], load_sem.at[1]),
        pltpu.make_async_copy(surface, sfb, load_sem.at[2]),
        pltpu.make_async_copy(lith, lit, load_sem.at[3]),
        pltpu.make_async_copy(w1h, w1, load_sem.at[4]),
        pltpu.make_async_copy(w5h, w5t, load_sem.at[5]),
        pltpu.make_async_copy(w2h, w2, load_sem.at[6]),
        pltpu.make_async_copy(w3h, w3, load_sem.at[7]),
        pltpu.make_async_copy(w4h, w4, load_sem.at[8]),
    ]
    for load in loads:
        load.start()

    barrier = pltpu.get_barrier_semaphore()

    def greet(dlat, dlon):
        pl.semaphore_signal(barrier, inc=1, device_id=at(dlat, dlon), device_id_type=MESH)

    for dlon in (-3, -2, -1, 1, 2, 3):
        greet(0, dlon)

    @pl.when(lat > 0)
    def _():
        for dlon in (-1, 0, 1):
            greet(-1, dlon)

    @pl.when(lat < N_LAT - 1)
    def _():
        for dlon in (-1, 0, 1):
            greet(1, dlon)

    loads[0].wait()
    shape = (LC, ROWS, COLS)
    lane = lax.broadcasted_iota(jnp.int32, shape, 2)
    sub = lax.broadcasted_iota(jnp.int32, shape, 1)
    for ch in range(NCH):
        z, m, p = (
            st[f * FIELD + ch * LC * ROWS : f * FIELD + (ch + 1) * LC * ROWS].reshape(shape) for f in range(3)
        )
        m = jnp.where(lat * ROWS + sub < N_LAT * ROWS - 1, m, 0.0)
        m_south = pltpu.roll(m, 1, 1)
        z_west = jnp.where(lane == 0, 0.0, pltpu.roll(z, 1, 2))
        d = COURANT * (z - z_west + m - jnp.where(sub == 0, 0.0, m_south))
        own_div[ch * LC * ROWS : (ch + 1) * LC * ROWS] = d.reshape(LC * ROWS, COLS)
        d_turned = pltpu.roll(d, 4, 1)
        to_south = jnp.where(sub < 4, p, d_turned)
        to_north = jnp.where(sub >= 4, p, jnp.where(sub >= 1, d_turned, m_south))
        rsend[0, ch] = to_south.reshape(LC * ROWS, COLS).astype(BF16)
        rsend[1, ch] = to_north.reshape(LC * ROWS, COLS).astype(BF16)
    lane2 = lax.broadcasted_iota(jnp.int32, (ROWS, COLS), 1)
    packed = []
    for f in range(3):
        for g in range(GROUPS):
            total = jnp.zeros((ROWS, COLS), F32)
            for kk in range(PER):
                row = (f * LEV + g * PER + kk) * ROWS
                total = jnp.where(lane2 // 8 == kk, pltpu.roll(st[row : row + ROWS], 4 + 8 * kk, 1), total)
            packed.append(total)
    own_edge[...] = jnp.concatenate(packed, axis=0)
    edges = own_edge[...]
    esend[...] = edges.astype(BF16)
    edges = edges.reshape(2, 3 * GROUPS // 2, ROWS, COLS)
    low, high = edges[0], edges[1]
    half = lax.broadcasted_iota(jnp.int32, low.shape, 1) < 4
    hsend[0] = jnp.where(half, low, pltpu.roll(high, 4, 1)).reshape(EROWS // 2, COLS).astype(BF16)
    hsend[1] = jnp.where(half, pltpu.roll(low, 4, 1), high).reshape(EROWS // 2, COLS).astype(BF16)

    neighbours = 6 + 3 * ((lat + N_LAT - 1) // N_LAT) + 3 * ((2 * N_LAT - 2 - lat) // N_LAT)
    pl.semaphore_wait(barrier, neighbours)

    def row_copy(side, ch):
        return pltpu.make_async_remote_copy(
            src_ref=rsend.at[side, ch], dst_ref=rrecv.at[side, ch],
            send_sem=rs_sem.at[side, ch], recv_sem=rr_sem.at[side, ch],
            device_id=at(2 * side - 1, 0), device_id_type=MESH,
        )

    def edge_copy(e):
        dlat, dlon = AROUND[e]
        place = AROUND.index((-dlat, -dlon))
        if dlat == 0:
            source, target = esend, erecv.at[place]
        else:
            source, target = hsend.at[(dlat + 1) // 2], hrecv.at[place - 2]
        return pltpu.make_async_remote_copy(
            src_ref=source, dst_ref=target,
            send_sem=es_sem.at[e], recv_sem=er_sem.at[place],
            device_id=at(dlat, dlon), device_id_type=MESH,
        )

    to_south, to_north = (2, 4, 5), (3, 6, 7)

    def all_edges(act):
        @pl.when(lat > 0)
        def _():
            for e in to_south:
                act(edge_copy(e))

        @pl.when(lat < N_LAT - 1)
        def _():
            for e in to_north:
                act(edge_copy(e))

        act(edge_copy(0))
        act(edge_copy(1))

    all_edges(lambda copy: copy.start())
    for ch in range(NCH):

        @pl.when(lat > 0)
        def _():
            row_copy(0, ch).start()

        @pl.when(lat < N_LAT - 1)
        def _():
            row_copy(1, ch).start()

    @pl.when(lat == 0)
    def _():
        rrecv[1] = jnp.zeros(rrecv.shape[1:], BF16)
        for e in to_south:
            hrecv[e - 2] = jnp.zeros(hrecv.shape[1:], BF16)

    @pl.when(lat == N_LAT - 1)
    def _():
        rrecv[0] = jnp.zeros(rrecv.shape[1:], BF16)
        for e in to_north:
            hrecv[e - 2] = jnp.zeros(hrecv.shape[1:], BF16)

    def block(n, slot):
        if isinstance(n, int) and n == OZ:
            return oz.at[slot]
        return qb.at[slot, n]

    def send(n, flow, source, slot, dlon):
        return pltpu.make_async_remote_copy(
            src_ref=block(n, source), dst_ref=block(n, slot),
            send_sem=qs_sem.at[n, flow], recv_sem=qr_sem.at[n, slot],
            device_id=at(0, dlon), device_id_type=MESH,
        )

    def first_hops(n, act):
        @pl.when(core == 0)
        def _():
            act(send(n, 0, 0, 2, 2))
            act(send(n, 1, 0, 1, 1))

        @pl.when(core == 1)
        def _():
            act(send(n, 0, 0, 3, 3))

        @pl.when(quarter == 1)
        def _():
            act(send(n, 1, 0, 2, 2))

    def arrived(n, slot):
        send(n, 0, 0, slot, 1).wait_recv()

    def forward(n):
        @pl.when(core == 0)
        def _():
            arrived(n, 3)

        @pl.when(quarter == 2)
        def _():
            send(n, 2, 3, 2, -1).start()

        arrived(n, 2)

        @pl.when(core == 0)
        def _():
            send(n, 3, 2, 3, 1).start()

        @pl.when(core == 1)
        def _():
            send(n, 3, 2, 1, -1).start()

    def complete(n):
        arrived(n, 1)

        @pl.when(core == 1)
        def _():
            arrived(n, 3)

    def drain(n):
        first_hops(n, lambda copy: copy.wait_send())

        @pl.when(quarter == 2)
        def _():
            send(n, 2, 3, 2, -1).wait_send()

        @pl.when(core == 0)
        def _():
            send(n, 3, 2, 3, 1).wait_send()

        @pl.when(core == 1)
        def _():
            send(n, 3, 2, 1, -1).wait_send()

    loads[1].wait()
    for j in range(ROWS):
        oz[0, j] = st[pl.ds(7 * FIELD + j, LEV, stride=ROWS), :].astype(BF16)
    first_hops(OZ, lambda copy: copy.start())
    loads[2].wait()
    sf[...] = sfb[...].astype(F32)
    loads[3].wait()
    listed = lit[...]
    row_id = lax.broadcasted_iota(jnp.int32, (ROWS, COLS), 0)
    col_id = lax.broadcasted_iota(jnp.int32, (COLS, COLS), 0)
    in_row, in_col = [], []
    for r in range(ROWS):
        entry = listed[r : r + 1]
        in_row.append(jnp.where(jnp.broadcast_to(entry >> 7, (ROWS, COLS)) == row_id, 1.0, 0.0))
        in_col.append(jnp.where(jnp.broadcast_to(entry & 127, (COLS, COLS)) == col_id, 1.0, 0.0))
    mask[...] = nt(jnp.concatenate(in_row, 1).astype(BF16), jnp.concatenate(in_col, 1).astype(BF16))
    loads[4].wait()
    eye_c = eye(COLS)

    def static_rows(j, carry):
        tracers = st[pl.ds(DYN * ROWS + j, 8 * LEV - DYN, stride=ROWS), :]
        ground = sf[pl.ds(j, 76, stride=ROWS), :]
        x = jnp.concatenate([tracers, ground], axis=0).astype(BF16)
        xt = nt(eye_c, x).astype(BF16)
        spot = pl.ds(pl.multiple_of(j * COLS, COLS), COLS)
        acc[spot, :] = jnp.dot(xt, w1[DYN:NIN], preferred_element_type=F32)
        return carry

    lax.fori_loop(0, ROWS, static_rows, 0)
    loads[5].wait()

    def edge_arrival(place):
        dlat, dlon = AROUND[place]
        if dlat == 0:
            source, target = esend, erecv.at[place]
        else:
            source, target = hsend.at[0], hrecv.at[place - 2]
        return pltpu.make_async_remote_copy(
            src_ref=source, dst_ref=target, send_sem=es_sem.at[place], recv_sem=er_sem.at[place],
            device_id=at(dlat, dlon), device_id_type=MESH,
        )

    @pl.when(lat > 0)
    def _():
        for e in to_south:
            edge_arrival(e).wait_recv()

    @pl.when(lat < N_LAT - 1)
    def _():
        for e in to_north:
            edge_arrival(e).wait_recv()

    edge_arrival(0).wait_recv()
    edge_arrival(1).wait_recv()

    strip_shape = (2 * GROUPS, ROWS, COLS)
    s_lane = lax.broadcasted_iota(jnp.int32, strip_shape, 2) % 8
    s_sub = lax.broadcasted_iota(jnp.int32, strip_shape, 1)
    group_shape = (3 * GROUPS, ROWS, COLS)
    first_half = lax.broadcasted_iota(jnp.int32, group_shape, 2) % 8 < 4

    def opened(sub):
        row_a = lat * ROWS + sub
        row_b = lat * ROWS + jnp.where(sub < 4, sub + ROWS, sub - ROWS)
        return row_a < N_LAT * ROWS - 1, jnp.logical_and(row_b >= 0, row_b < N_LAT * ROWS - 1)

    def beyond(north_place, south_place):
        nn = hrecv[north_place - 2].astype(F32).reshape(half.shape)
        ss = hrecv[south_place - 2].astype(F32).reshape(half.shape)
        return jnp.concatenate(
            [jnp.where(half, nn, pltpu.roll(ss, 4, 1)), jnp.where(half, pltpu.roll(nn, 4, 1), ss)], axis=0
        )

    def strips(west_edge, middle, east_edge):
        on_east, on_west = jnp.where(first_half, middle, east_edge), jnp.where(first_half, west_edge, middle)
        return [
            jnp.concatenate([on_east[f * GROUPS : (f + 1) * GROUPS], on_west[f * GROUPS : (f + 1) * GROUPS]], axis=0)
            for f in range(3)
        ]

    za, ma, pa = strips(
        erecv[0].astype(F32).reshape(group_shape), own_edge[...].reshape(group_shape), erecv[1].astype(F32).reshape(group_shape)
    )
    zb, mb, pb = strips(beyond(6, 4), beyond(3, 2), beyond(7, 5))

    def turn(x, steps):
        return pltpu.roll(x, steps % COLS, 2)

    def north(sub, x, y):
        x, y = pltpu.roll(x, ROWS - 1, 1), pltpu.roll(y, ROWS - 1, 1)
        return jnp.where(sub == ROWS - 1, y, x), jnp.where(sub == ROWS - 1, x, y)

    def south(sub, x, y):
        x, y = pltpu.roll(x, 1, 1), pltpu.roll(y, 1, 1)
        return jnp.where(sub == 0, y, x), jnp.where(sub == 0, x, y)

    def hand(index, value):
        merged = jnp.where(s_lane[:GROUPS] == 2, turn(value[:GROUPS], -2), value[GROUPS:])
        give[index] = merged.reshape(GROUPS * ROWS, COLS)

    square = COURANT * COURANT
    open_a, open_b = opened(s_sub)
    ma, mb = jnp.where(open_a, ma, 0.0), jnp.where(open_b, mb, 0.0)
    msa, msb = south(s_sub, ma, mb)
    da = COURANT * (za - turn(za, 1) + ma - msa)
    db = COURANT * (zb - turn(zb, 1) + mb - msb)
    hand(ZA, COURANT * za)
    hand(ZB, COURANT * zb)
    sa, sb = pa, pb
    for step in range(4):
        hand(A1 + step, sa)
        if step < 3:
            hand(B1 + step, sb)
            na, nb = north(s_sub, sa, sb)
            ga, gb = jnp.where(open_a, na - sa, 0.0), jnp.where(open_b, nb - sb, 0.0)
            gsa, gsb = south(s_sub, ga, gb)
            pa = pa - da + square * (turn(sa, -1) + turn(sa, 1) - 2.0 * sa + ga - gsa)
            pb = pb - db + square * (turn(sb, -1) + turn(sb, 1) - 2.0 * sb + gb - gsb)
            sa, sb = sa + pa, sb + pb
    hand(ZF, za - COURANT * (turn(sa, -1) - sa))

    open_a, open_b = opened(sub)
    first_lane, last_lane = lane == 0, lane == COLS - 1

    def acoustic(ch, carry):
        @pl.when(lat > 0)
        def _():
            row_copy(1, ch).wait_recv()

        @pl.when(lat < N_LAT - 1)
        def _():
            row_copy(0, ch).wait_recv()

        def spot_of(f):
            return pl.ds(pl.multiple_of(f * FIELD + ch * LC * ROWS, ROWS), LC * ROWS)

        def given(index):
            pieces = []
            for g in range(LC // PER):
                group = give[index, pl.ds(pl.multiple_of((ch * (LC // PER) + g) * ROWS, ROWS), ROWS), :]
                for kk in range(PER):
                    pieces.append(pltpu.roll(group, (COLS - 3 - 8 * kk) % COLS, 1).reshape(1, ROWS, COLS))
            return jnp.concatenate(pieces, axis=0)

        def sides(x, other):
            return jnp.where(last_lane, other, turn(x, -1)) + jnp.where(first_lane, other, turn(x, 1))

        from_north = rrecv[0, ch].astype(F32).reshape(shape)
        from_south = rrecv[1, ch].astype(F32).reshape(shape)
        pb = jnp.where(sub < 4, from_north, from_south)
        db = pltpu.roll(jnp.where(sub < 4, from_south, from_north), 4, 1)
        ma = jnp.where(open_a, st[spot_of(1), :].reshape(shape), 0.0)
        db = db - jnp.where(first_lane, given(ZB), 0.0) - jnp.where(sub == 0, COURANT * pltpu.roll(ma, 1, 1), 0.0)
        da = own_div[spot_of(0), :].reshape(shape)
        da = da - jnp.where(first_lane, given(ZA), 0.0) - jnp.where(sub == 0, COURANT * from_south, 0.0)
        pa = st[spot_of(2), :].reshape(shape)
        sa, sb = pa, pb
        for step in range(4):
            na, nb = north(sub, sa, sb)
            ga, gb = jnp.where(open_a, na - sa, 0.0), jnp.where(open_b, nb - sb, 0.0)
            gsa, gsb = south(sub, ga, gb)
            other = given(A1 + step)
            if step == 3:
                ea = jnp.where(last_lane, other, turn(sa, -1))
                across = ea + jnp.where(first_lane, other, turn(sa, 1))
            else:
                across = sides(sa, other)
            pa = pa - da + square * (across - 2.0 * sa + ga - gsa)
            if step < 3:
                pb = pb - db + square * (sides(sb, given(B1 + step)) - 2.0 * sb + gb - gsb)
                sa, sb = sa + pa, sb + pb
        za = st[spot_of(0), :].reshape(shape) - COURANT * (ea - sa)
        ma = jnp.where(open_a, ma - COURANT * ga, 0.0)
        z_west = jnp.where(first_lane, given(ZF), turn(za, 1))
        share = (0.5 + 0.45 * jnp.tanh(za)).reshape(LC * ROWS, COLS)
        share_west = (0.5 + 0.45 * jnp.tanh(z_west)).reshape(LC * ROWS, COLS)
        for f, value in enumerate((za, ma, pa)):
            st[spot_of(f), :] = value.reshape(LC * ROWS, COLS)
        out[spot_of(2), :] = pa.reshape(LC * ROWS, COLS)
        for f in range(4):
            fr[spot_of(f), :] = share
            fw[spot_of(f), :] = share_west
        return carry

    lax.fori_loop(0, NCH, acoustic, 0)

    for load in loads[6:]:
        load.wait()

    def network(n, carry):
        xs = []
        for r in range(CH):
            x = st[pl.ds(n * CH + r, DYN, stride=ROWS), :].astype(BF16)
            xs.append(nt(eye_c, x).astype(BF16))
        xt = jnp.concatenate(xs, axis=0)
        spot = pl.ds(pl.multiple_of(n * CH * COLS, COLS), CH * COLS)
        h = leaky(acc[spot, :] + jnp.dot(xt, w1[0:DYN], preferred_element_type=F32))
        for w in (w2, w3, w4):
            h = leaky(jnp.dot(h, w[...], preferred_element_type=F32))
        y = nt(w5t[...], h)
        for r in range(CH):
            j = n * CH + r
            t = jnp.where(jnp.broadcast_to(mask[pl.ds(j, 1), :], (NOUT, COLS)) > 0.5, y[:, r * COLS : (r + 1) * COLS], 0.0)
            out[pl.ds(j, 2 * LEV, stride=ROWS), :] = st[pl.ds(j, 2 * LEV, stride=ROWS), :] + STEP * t[0 : 2 * LEV]
            q = st[pl.ds(3 * FIELD + j, 4 * LEV, stride=ROWS), :] + STEP * t[2 * LEV : 6 * LEV]
            qb[0, j] = q.astype(BF16)
            fl[pl.ds(j, 8, stride=ROWS), :] = t[6 * LEV :]
        for r in range(CH):
            first_hops(n * CH + r, lambda copy: copy.start())
        return carry

    lax.fori_loop(0, NB, network, 0)
    flux[...] = fl[...].astype(BF16)

    def advect(j, ref, count, base):
        offset = off[j]
        tiles, cells = offset >> 7, offset & 127
        tile_shape = (count, COLS)
        where = lax.broadcasted_iota(jnp.int32, tile_shape, 1)
        parts = [ref[slot, j].astype(F32) for slot in range(4)]

        def pick(cut):
            d = tiles + jnp.where(where >= cut, 1, 0)
            return jnp.where(d == 0, parts[0], jnp.where(d == 1, parts[1], jnp.where(d == 2, parts[2], parts[3])))

        near = pltpu.roll(pick(COLS - cells), cells, 1)
        far = pltpu.roll(pick(COLS - 1 - cells), (cells + 1) & 127, 1)
        spot = pl.ds(j, count, stride=ROWS)
        value = (1.0 - fr[spot, :]) * near + fw[spot, :] * far
        out[pl.ds(base * FIELD + j, count, stride=ROWS), :] = value

    forward(OZ)

    def tracer_row(n, carry):
        forward(n)

        @pl.when(n > 0)
        def _():
            complete(n - 1)
            advect(n - 1, qb, 4 * LEV, 3)

        return carry

    complete(OZ)

    def ozone_row(j, carry):
        advect(j, oz, LEV, 7)
        return carry

    lax.fori_loop(0, ROWS, ozone_row, 0)
    lax.fori_loop(0, ROWS, tracer_row, 0)
    complete(ROWS - 1)
    advect(ROWS - 1, qb, 4 * LEV, 3)

    all_edges(lambda copy: copy.wait_send())
    for ch in range(NCH):

        @pl.when(lat > 0)
        def _():
            row_copy(0, ch).wait_send()

        @pl.when(lat < N_LAT - 1)
        def _():
            row_copy(1, ch).wait_send()

    drain(OZ)

    def drain_block(n, carry):
        drain(n)
        return carry

    lax.fori_loop(0, ROWS, drain_block, 0)


def place(state, flux, state_out, flux_out, sem):
    copies = [pltpu.make_async_copy(flux, flux_out, sem.at[4])]
    for part in range(4):
        spot = slice(part * 2 * FIELD, (part + 1) * 2 * FIELD)
        copies.append(pltpu.make_async_copy(state.at[spot], state_out.at[spot], sem.at[part]))
    for copy in copies:
        copy.start()
    for copy in copies:
        copy.wait()


def on_device(state, surface, layer_one, layer_two, layer_three, layer_four, layer_five, lit_columns, row_offset):
    fields = state.shape[0]
    any_spec = pl.BlockSpec(memory_space=pl.ANY)
    vmem_spec = pl.BlockSpec(memory_space=pltpu.VMEM)
    dma = pltpu.SemaphoreType.DMA
    new_state, surface_flux = pl.pallas_call(
        kernel,
        out_shape=(
            pltpu.VMEM((fields * FIELD, COLS), F32),
            pltpu.VMEM((8 * ROWS, COLS), BF16),
        ),
        in_specs=[any_spec] * 8 + [pl.BlockSpec(memory_space=pltpu.SMEM)],
        out_specs=(vmem_spec, vmem_spec),
        scratch_shapes=[
            pltpu.VMEM((fields * FIELD, COLS), F32),
            pltpu.VMEM((76 * ROWS, COLS), BF16),
            pltpu.VMEM((76 * ROWS, COLS), F32),
            pltpu.VMEM((NIN, H1), BF16),
            pltpu.VMEM((H1, H2), BF16),
            pltpu.VMEM((H2, H3), BF16),
            pltpu.VMEM((H3, H4), BF16),
            pltpu.VMEM((NOUT, H4), BF16),
            pltpu.VMEM((ROWS, COLS), jnp.int32),
            pltpu.VMEM((ROWS * COLS, H1), F32),
            pltpu.VMEM((ROWS, COLS), F32),
            pltpu.VMEM((4 * FIELD, COLS), F32),
            pltpu.VMEM((4 * FIELD, COLS), F32),
            pltpu.VMEM((8 * ROWS, COLS), F32),
            pltpu.VMEM((FIELD, COLS), F32),
            pltpu.VMEM((2, NCH, LC * ROWS, COLS), BF16),
            pltpu.VMEM((2, NCH, LC * ROWS, COLS), BF16),
            pltpu.VMEM((EROWS, COLS), F32),
            pltpu.VMEM((EROWS, COLS), BF16),
            pltpu.VMEM((2, EROWS // 2, COLS), BF16),
            pltpu.VMEM((2, EROWS, COLS), BF16),
            pltpu.VMEM((6, EROWS // 2, COLS), BF16),
            pltpu.VMEM((10, GROUPS * ROWS, COLS), F32),
            pltpu.VMEM((4, ROWS, LEV, COLS), BF16),
            pltpu.VMEM((4, ROWS, 4 * LEV, COLS), BF16),
            dma((9,)),
            dma((2, NCH)),
            dma((2, NCH)),
            dma((8,)),
            dma((8,)),
            dma((ROWS + 1, 4)),
            dma((ROWS + 1, 4)),
        ],
        compiler_params=pltpu.CompilerParams(
            collective_id=0, has_side_effects=True, vmem_limit_bytes=56 * 1024 * 1024
        ),
    )(
        state.reshape(fields * FIELD, COLS),
        surface.reshape(76 * ROWS, COLS),
        layer_one, layer_two, layer_three, layer_four, layer_five.T,
        lit_columns.reshape(ROWS, COLS),
        row_offset,
    )
    new_state, surface_flux = pl.pallas_call(
        place,
        out_shape=(
            jax.ShapeDtypeStruct((fields * FIELD, COLS), F32),
            jax.ShapeDtypeStruct((8 * ROWS, COLS), BF16),
        ),
        in_specs=[vmem_spec, vmem_spec],
        out_specs=(any_spec, any_spec),
        scratch_shapes=[dma((5,))],
    )(pltpu.with_memory_space_constraint(new_state, pltpu.VMEM), pltpu.with_memory_space_constraint(surface_flux, pltpu.VMEM))
    return new_state.reshape(fields, LEV, ROWS, COLS), surface_flux.reshape(8, ROWS, COLS)


def solution(mesh):
    in_specs = (
        P(None, None, "lat", "lon"), P(None, "lat", "lon"), P(), P(), P(), P(), P(), P("lat", "lon", None), P("lat"),
    )
    out_specs = (P(None, None, "lat", "lon"), P(None, "lat", "lon"))
    return jax.shard_map(on_device, mesh=mesh, in_specs=in_specs, out_specs=out_specs, check_vma=False)
```

```python
import jax
import jax.numpy as jnp
from jax import lax
from jax.experimental import pallas as pl
from jax.experimental.pallas import tpu as pltpu
from jax.sharding import PartitionSpec as P

MESH = pl.DeviceIdType.MESH
F32, BF16 = jnp.float32, jnp.bfloat16

N_LAT, N_LON = 8, 16
LEV = 60
ROWS, COLS = 8, 128
FIELD = LEV * ROWS
COURANT = 0.6
STEP = 0.5
SLOPE = 0.15
DYN = 192
NIN, NOUT = 556, 368
H1, H2, H3, H4 = 768, 640, 512, 640

LC = 30
NCH = LEV // LC
PER = 15
GROUPS = LEV // PER
EROWS = 3 * GROUPS * ROWS
CH = 2
LAG_B, LAG_C = 1, 2
NB = ROWS // CH
OZ = NB

AROUND = ((0, -1), (0, 1), (-1, 0), (1, 0), (-1, -1), (-1, 1), (1, -1), (1, 1))
A1, B1, ZA, ZB, ZF = 0, 4, 7, 8, 9


def nt(a, b):
    return lax.dot_general(a, b, (((1,), (1,)), ((), ())), preferred_element_type=F32)


def eye(n):
    return (lax.broadcasted_iota(jnp.int32, (n, n), 0) == lax.broadcasted_iota(jnp.int32, (n, n), 1)).astype(F32).astype(BF16)


def leaky(z):
    return jnp.maximum(z, SLOPE * z).astype(BF16)


def kernel(
    state, surface, w1h, w2h, w3h, w4h, w5h, lith, off,
    out, flux,
    st, sfb, sf, w1, w2, w3, w4, w5t, lit, acc, mask, fr, fw, fl,
    own_div, rsend, rrecv, own_edge, esend, hsend, erecv, hrecv, give, oz, qb,
    load_sem, rs_sem, rr_sem, es_sem, er_sem, qs_sem, qr_sem,
):
    lat, lon = lax.axis_index("lat"), lax.axis_index("lon")
    core, quarter = lax.rem(lon, 2), lax.rem(lon, 4)

    def at(dlat, dlon):
        return (lat + dlat, lax.rem(lon + dlon + N_LON, N_LON))

    loads = [
        pltpu.make_async_copy(state.at[0 : 3 * FIELD], st.at[0 : 3 * FIELD], load_sem.at[0]),
        pltpu.make_async_copy(state.at[3 * FIELD : 8 * FIELD], st.at[3 * FIELD : 8 * FIELD], load_sem.at[1]),
        pltpu.make_async_copy(surface, sfb, load_sem.at[2]),
        pltpu.make_async_copy(lith, lit, load_sem.at[3]),
        pltpu.make_async_copy(w1h, w1, load_sem.at[4]),
        pltpu.make_async_copy(w5h, w5t, load_sem.at[5]),
        pltpu.make_async_copy(w2h, w2, load_sem.at[6]),
        pltpu.make_async_copy(w3h, w3, load_sem.at[7]),
        pltpu.make_async_copy(w4h, w4, load_sem.at[8]),
    ]
    for load in loads:
        load.start()

    barrier = pltpu.get_barrier_semaphore()

    def greet(dlat, dlon):
        pl.semaphore_signal(barrier, inc=1, device_id=at(dlat, dlon), device_id_type=MESH)

    for dlon in (-4, -3, -2, -1, 1, 2, 3, 4):
        greet(0, dlon)

    @pl.when(lat > 0)
    def _():
        for dlon in (-1, 0, 1):
            greet(-1, dlon)

    @pl.when(lat < N_LAT - 1)
    def _():
        for dlon in (-1, 0, 1):
            greet(1, dlon)

    loads[0].wait()
    shape = (LC, ROWS, COLS)
    lane = lax.broadcasted_iota(jnp.int32, shape, 2)
    sub = lax.broadcasted_iota(jnp.int32, shape, 1)
    for ch in range(NCH):
        z, m, p = (
            st[f * FIELD + ch * LC * ROWS : f * FIELD + (ch + 1) * LC * ROWS].reshape(shape) for f in range(3)
        )
        m = jnp.where(lat * ROWS + sub < N_LAT * ROWS - 1, m, 0.0)
        m_south = pltpu.roll(m, 1, 1)
        z_west = jnp.where(lane == 0, 0.0, pltpu.roll(z, 1, 2))
        d = COURANT * (z - z_west + m - jnp.where(sub == 0, 0.0, m_south))
        own_div[ch * LC * ROWS : (ch + 1) * LC * ROWS] = d.reshape(LC * ROWS, COLS)
        d_turned = pltpu.roll(d, 4, 1)
        to_south = jnp.where(sub < 4, p, d_turned)
        to_north = jnp.where(sub >= 4, p, jnp.where(sub >= 1, d_turned, m_south))
        rsend[0, ch] = to_south.reshape(LC * ROWS, COLS).astype(BF16)
        rsend[1, ch] = to_north.reshape(LC * ROWS, COLS).astype(BF16)
    lane2 = lax.broadcasted_iota(jnp.int32, (ROWS, COLS), 1)
    packed = []
    for f in range(3):
        for g in range(GROUPS):
            total = jnp.zeros((ROWS, COLS), F32)
            for kk in range(PER):
                row = (f * LEV + g * PER + kk) * ROWS
                total = jnp.where(lane2 // 8 == kk, pltpu.roll(st[row : row + ROWS], 4 + 8 * kk, 1), total)
            packed.append(total)
    own_edge[...] = jnp.concatenate(packed, axis=0)
    edges = own_edge[...]
    esend[...] = edges.astype(BF16)
    edges = edges.reshape(2, 3 * GROUPS // 2, ROWS, COLS)
    low, high = edges[0], edges[1]
    half = lax.broadcasted_iota(jnp.int32, low.shape, 1) < 4
    hsend[0] = jnp.where(half, low, pltpu.roll(high, 4, 1)).reshape(EROWS // 2, COLS).astype(BF16)
    hsend[1] = jnp.where(half, pltpu.roll(low, 4, 1), high).reshape(EROWS // 2, COLS).astype(BF16)

    neighbours = 8 + 3 * ((lat + N_LAT - 1) // N_LAT) + 3 * ((2 * N_LAT - 2 - lat) // N_LAT)
    pl.semaphore_wait(barrier, neighbours)

    def row_copy(side, ch):
        return pltpu.make_async_remote_copy(
            src_ref=rsend.at[side, ch], dst_ref=rrecv.at[side, ch],
            send_sem=rs_sem.at[side, ch], recv_sem=rr_sem.at[side, ch],
            device_id=at(2 * side - 1, 0), device_id_type=MESH,
        )

    def edge_copy(e):
        dlat, dlon = AROUND[e]
        place = AROUND.index((-dlat, -dlon))
        if dlat == 0:
            source, target = esend, erecv.at[place]
        else:
            source, target = hsend.at[(dlat + 1) // 2], hrecv.at[place - 2]
        return pltpu.make_async_remote_copy(
            src_ref=source, dst_ref=target,
            send_sem=es_sem.at[e], recv_sem=er_sem.at[place],
            device_id=at(dlat, dlon), device_id_type=MESH,
        )

    to_south, to_north = (2, 4, 5), (3, 6, 7)

    def all_edges(act):
        @pl.when(lat > 0)
        def _():
            for e in to_south:
                act(edge_copy(e))

        @pl.when(lat < N_LAT - 1)
        def _():
            for e in to_north:
                act(edge_copy(e))

        act(edge_copy(0))
        act(edge_copy(1))

    all_edges(lambda copy: copy.start())
    for ch in range(NCH):

        @pl.when(lat > 0)
        def _():
            row_copy(0, ch).start()

        @pl.when(lat < N_LAT - 1)
        def _():
            row_copy(1, ch).start()

    @pl.when(lat == 0)
    def _():
        rrecv[1] = jnp.zeros(rrecv.shape[1:], BF16)
        for e in to_south:
            hrecv[e - 2] = jnp.zeros(hrecv.shape[1:], BF16)

    @pl.when(lat == N_LAT - 1)
    def _():
        rrecv[0] = jnp.zeros(rrecv.shape[1:], BF16)
        for e in to_north:
            hrecv[e - 2] = jnp.zeros(hrecv.shape[1:], BF16)

    def block(n, slot):
        if isinstance(n, int) and n == OZ:
            return oz.at[slot]
        return qb.at[slot, pl.ds(n * CH, CH)]

    def send(n, flow, source, slot, dlon):
        return pltpu.make_async_remote_copy(
            src_ref=block(n, source), dst_ref=block(n, slot),
            send_sem=qs_sem.at[n, flow], recv_sem=qr_sem.at[n, slot],
            device_id=at(0, dlon), device_id_type=MESH,
        )

    def flow(name, n):
        if name == "y" or name == "d":
            return send(n, 0 if name == "d" else 1, 0, 2, 2)
        if name == "z":
            return send(n, 0, 0, 3, 3)
        if name == "x":
            return send(n, 0, 0, 4, 4)
        if name == "s":
            return send(n, 1, 4, 3, -1)
        if name == "p":
            return send(n, 2, 0, 1, 1)
        if name == "r":
            return send(n, 3, 4, 2, -2)
        if name == "f":
            return send(n, 4, 2, 3, 1)
        return send(n, 4, 2, 1, -1)

    sources = {
        "y": quarter < 2, "d": quarter == 2, "z": quarter == 1, "x": quarter == 3, "p": core == 0,
        "r": quarter == 3, "s": quarter == 3, "f": core == 0, "g": quarter == 3, "h": quarter == 1,
    }
    drains = {
        "y": quarter >= 2, "d": quarter == 0, "z": quarter == 0, "x": quarter == 3, "p": core == 1,
        "r": quarter == 1, "s": quarter == 2, "f": core == 1, "g": quarter == 2, "h": quarter == 0,
    }

    def do(name, n, act):
        @pl.when(sources[name])
        def _():
            act(flow(name, n))

    def got(name, n):
        @pl.when(drains[name])
        def _():
            flow(name, n).wait_recv()

    def first_hops(n, act):
        for name in "xdyzp":
            do(name, n, act)

    def begin(copy):
        copy.start()

    def relay(n):
        got("x", n)
        do("r", n, begin)
        do("s", n, begin)

    def forward(n):
        got("d", n)
        got("y", n)
        do("f", n, begin)
        do("g", n, begin)

    def forward_relayed(n):
        got("r", n)
        do("h", n, begin)

    def complete(n):
        got("z", n)
        got("s", n)
        got("p", n)
        got("g", n)
        got("h", n)
        got("f", n)

    def drain(n):
        for name in "ydzxprsfgh":
            do(name, n, lambda copy: copy.wait_send())

    loads[1].wait()
    for j in range(ROWS):
        oz[0, j] = st[pl.ds(7 * FIELD + j, LEV, stride=ROWS), :].astype(BF16)
    first_hops(OZ, lambda copy: copy.start())
    loads[2].wait()
    sf[...] = sfb[...].astype(F32)
    loads[3].wait()
    listed = lit[...]
    row_id = lax.broadcasted_iota(jnp.int32, (ROWS, COLS), 0)
    col_id = lax.broadcasted_iota(jnp.int32, (COLS, COLS), 0)
    in_row, in_col = [], []
    for r in range(ROWS):
        entry = listed[r : r + 1]
        in_row.append(jnp.where(jnp.broadcast_to(entry >> 7, (ROWS, COLS)) == row_id, 1.0, 0.0))
        in_col.append(jnp.where(jnp.broadcast_to(entry & 127, (COLS, COLS)) == col_id, 1.0, 0.0))
    mask[...] = nt(jnp.concatenate(in_row, 1).astype(BF16), jnp.concatenate(in_col, 1).astype(BF16))
    loads[4].wait()
    eye_c = eye(COLS)

    def static_rows(j, carry):
        tracers = st[pl.ds(DYN * ROWS + j, 8 * LEV - DYN, stride=ROWS), :]
        ground = sf[pl.ds(j, 76, stride=ROWS), :]
        x = jnp.concatenate([tracers, ground], axis=0).astype(BF16)
        xt = nt(eye_c, x).astype(BF16)
        spot = pl.ds(pl.multiple_of(j * COLS, COLS), COLS)
        acc[spot, :] = jnp.dot(xt, w1[DYN:NIN], preferred_element_type=F32)
        return carry

    lax.fori_loop(0, ROWS, static_rows, 0)
    loads[5].wait()

    def edge_arrival(place):
        dlat, dlon = AROUND[place]
        if dlat == 0:
            source, target = esend, erecv.at[place]
        else:
            source, target = hsend.at[0], hrecv.at[place - 2]
        return pltpu.make_async_remote_copy(
            src_ref=source, dst_ref=target, send_sem=es_sem.at[place], recv_sem=er_sem.at[place],
            device_id=at(dlat, dlon), device_id_type=MESH,
        )

    @pl.when(lat > 0)
    def _():
        for e in to_south:
            edge_arrival(e).wait_recv()

    @pl.when(lat < N_LAT - 1)
    def _():
        for e in to_north:
            edge_arrival(e).wait_recv()

    edge_arrival(0).wait_recv()
    edge_arrival(1).wait_recv()

    strip_shape = (2 * GROUPS, ROWS, COLS)
    s_lane = lax.broadcasted_iota(jnp.int32, strip_shape, 2) % 8
    s_sub = lax.broadcasted_iota(jnp.int32, strip_shape, 1)
    group_shape = (3 * GROUPS, ROWS, COLS)
    first_half = lax.broadcasted_iota(jnp.int32, group_shape, 2) % 8 < 4

    def opened(sub):
        row_a = lat * ROWS + sub
        row_b = lat * ROWS + jnp.where(sub < 4, sub + ROWS, sub - ROWS)
        return row_a < N_LAT * ROWS - 1, jnp.logical_and(row_b >= 0, row_b < N_LAT * ROWS - 1)

    def beyond(north_place, south_place):
        nn = hrecv[north_place - 2].astype(F32).reshape(half.shape)
        ss = hrecv[south_place - 2].astype(F32).reshape(half.shape)
        return jnp.concatenate(
            [jnp.where(half, nn, pltpu.roll(ss, 4, 1)), jnp.where(half, pltpu.roll(nn, 4, 1), ss)], axis=0
        )

    def strips(west_edge, middle, east_edge):
        on_east, on_west = jnp.where(first_half, middle, east_edge), jnp.where(first_half, west_edge, middle)
        return [
            jnp.concatenate([on_east[f * GROUPS : (f + 1) * GROUPS], on_west[f * GROUPS : (f + 1) * GROUPS]], axis=0)
            for f in range(3)
        ]

    za, ma, pa = strips(
        erecv[0].astype(F32).reshape(group_shape), own_edge[...].reshape(group_shape), erecv[1].astype(F32).reshape(group_shape)
    )
    zb, mb, pb = strips(beyond(6, 4), beyond(3, 2), beyond(7, 5))

    def turn(x, steps):
        return pltpu.roll(x, steps % COLS, 2)

    def north(sub, x, y):
        x, y = pltpu.roll(x, ROWS - 1, 1), pltpu.roll(y, ROWS - 1, 1)
        return jnp.where(sub == ROWS - 1, y, x), jnp.where(sub == ROWS - 1, x, y)

    def south(sub, x, y):
        x, y = pltpu.roll(x, 1, 1), pltpu.roll(y, 1, 1)
        return jnp.where(sub == 0, y, x), jnp.where(sub == 0, x, y)

    def hand(index, value):
        merged = jnp.where(s_lane[:GROUPS] == 2, turn(value[:GROUPS], -2), value[GROUPS:])
        give[index] = merged.reshape(GROUPS * ROWS, COLS)

    square = COURANT * COURANT
    open_a, open_b = opened(s_sub)
    ma, mb = jnp.where(open_a, ma, 0.0), jnp.where(open_b, mb, 0.0)
    msa, msb = south(s_sub, ma, mb)
    da = COURANT * (za - turn(za, 1) + ma - msa)
    db = COURANT * (zb - turn(zb, 1) + mb - msb)
    hand(ZA, COURANT * za)
    hand(ZB, COURANT * zb)
    sa, sb = pa, pb
    for step in range(4):
        hand(A1 + step, sa)
        if step < 3:
            hand(B1 + step, sb)
            na, nb = north(s_sub, sa, sb)
            ga, gb = jnp.where(open_a, na - sa, 0.0), jnp.where(open_b, nb - sb, 0.0)
            gsa, gsb = south(s_sub, ga, gb)
            pa = pa - da + square * (turn(sa, -1) + turn(sa, 1) - 2.0 * sa + ga - gsa)
            pb = pb - db + square * (turn(sb, -1) + turn(sb, 1) - 2.0 * sb + gb - gsb)
            sa, sb = sa + pa, sb + pb
    hand(ZF, za - COURANT * (turn(sa, -1) - sa))

    open_a, open_b = opened(sub)
    first_lane, last_lane = lane == 0, lane == COLS - 1

    def acoustic(ch, carry):
        @pl.when(lat > 0)
        def _():
            row_copy(1, ch).wait_recv()

        @pl.when(lat < N_LAT - 1)
        def _():
            row_copy(0, ch).wait_recv()

        def spot_of(f):
            return pl.ds(pl.multiple_of(f * FIELD + ch * LC * ROWS, ROWS), LC * ROWS)

        def given(index):
            pieces = []
            for g in range(LC // PER):
                group = give[index, pl.ds(pl.multiple_of((ch * (LC // PER) + g) * ROWS, ROWS), ROWS), :]
                for kk in range(PER):
                    pieces.append(pltpu.roll(group, (COLS - 3 - 8 * kk) % COLS, 1).reshape(1, ROWS, COLS))
            return jnp.concatenate(pieces, axis=0)

        def sides(x, other):
            return jnp.where(last_lane, other, turn(x, -1)) + jnp.where(first_lane, other, turn(x, 1))

        from_north = rrecv[0, ch].astype(F32).reshape(shape)
        from_south = rrecv[1, ch].astype(F32).reshape(shape)
        pb = jnp.where(sub < 4, from_north, from_south)
        db = pltpu.roll(jnp.where(sub < 4, from_south, from_north), 4, 1)
        ma = jnp.where(open_a, st[spot_of(1), :].reshape(shape), 0.0)
        db = db - jnp.where(first_lane, given(ZB), 0.0) - jnp.where(sub == 0, COURANT * pltpu.roll(ma, 1, 1), 0.0)
        da = own_div[spot_of(0), :].reshape(shape)
        da = da - jnp.where(first_lane, given(ZA), 0.0) - jnp.where(sub == 0, COURANT * from_south, 0.0)
        pa = st[spot_of(2), :].reshape(shape)
        sa, sb = pa, pb
        for step in range(4):
            na, nb = north(sub, sa, sb)
            ga, gb = jnp.where(open_a, na - sa, 0.0), jnp.where(open_b, nb - sb, 0.0)
            gsa, gsb = south(sub, ga, gb)
            other = given(A1 + step)
            if step == 3:
                ea = jnp.where(last_lane, other, turn(sa, -1))
                across = ea + jnp.where(first_lane, other, turn(sa, 1))
            else:
                across = sides(sa, other)
            pa = pa - da + square * (across - 2.0 * sa + ga - gsa)
            if step < 3:
                pb = pb - db + square * (sides(sb, given(B1 + step)) - 2.0 * sb + gb - gsb)
                sa, sb = sa + pa, sb + pb
        za = st[spot_of(0), :].reshape(shape) - COURANT * (ea - sa)
        ma = jnp.where(open_a, ma - COURANT * ga, 0.0)
        z_west = jnp.where(first_lane, given(ZF), turn(za, 1))
        share = (0.5 + 0.45 * jnp.tanh(za)).reshape(LC * ROWS, COLS)
        share_west = (0.5 + 0.45 * jnp.tanh(z_west)).reshape(LC * ROWS, COLS)
        for f, value in enumerate((za, ma, pa)):
            st[spot_of(f), :] = value.reshape(LC * ROWS, COLS)
        out[spot_of(2), :] = pa.reshape(LC * ROWS, COLS)
        for f in range(4):
            fr[spot_of(f), :] = share
            fw[spot_of(f), :] = share_west
        return carry

    lax.fori_loop(0, NCH, acoustic, 0)

    relay(OZ)
    forward(OZ)
    for load in loads[6:]:
        load.wait()

    def network(n, carry):
        xs = []
        for r in range(CH):
            x = st[pl.ds(n * CH + r, DYN, stride=ROWS), :].astype(BF16)
            xs.append(nt(eye_c, x).astype(BF16))
        xt = jnp.concatenate(xs, axis=0)
        spot = pl.ds(pl.multiple_of(n * CH * COLS, COLS), CH * COLS)
        h = leaky(acc[spot, :] + jnp.dot(xt, w1[0:DYN], preferred_element_type=F32))
        for w in (w2, w3, w4):
            h = leaky(jnp.dot(h, w[...], preferred_element_type=F32))
        y = nt(w5t[...], h)
        for r in range(CH):
            j = n * CH + r
            t = jnp.where(jnp.broadcast_to(mask[pl.ds(j, 1), :], (NOUT, COLS)) > 0.5, y[:, r * COLS : (r + 1) * COLS], 0.0)
            q = st[pl.ds(3 * FIELD + j, 4 * LEV, stride=ROWS), :] + STEP * t[2 * LEV : 6 * LEV]
            qb[0, j] = q.astype(BF16)
            out[pl.ds(j, 2 * LEV, stride=ROWS), :] = st[pl.ds(j, 2 * LEV, stride=ROWS), :] + STEP * t[0 : 2 * LEV]
            fl[pl.ds(j, 8, stride=ROWS), :] = t[6 * LEV :]
        first_hops(n, begin)
        return carry

    lax.fori_loop(0, ROWS // CH, network, 0)
    forward_relayed(OZ)

    @pl.when(quarter == 3)
    def _():
        def relay_row(n, carry):
            relay(n)
            return carry

        lax.fori_loop(0, NB, relay_row, 0)

    flux[...] = fl[...].astype(BF16)

    def advect(j, ref, count, base):
        offset = off[j]
        tiles, cells = offset >> 7, offset & 127
        tile_shape = (count, COLS)
        where = lax.broadcasted_iota(jnp.int32, tile_shape, 1)
        parts = [ref[slot, j].astype(F32) for slot in range(4)]

        def pick(cut):
            d = tiles + jnp.where(where >= cut, 1, 0)
            return jnp.where(d == 0, parts[0], jnp.where(d == 1, parts[1], jnp.where(d == 2, parts[2], parts[3])))

        near = pltpu.roll(pick(COLS - cells), cells, 1)
        far = pltpu.roll(pick(COLS - 1 - cells), (cells + 1) & 127, 1)
        spot = pl.ds(j, count, stride=ROWS)
        value = (1.0 - fr[spot, :]) * near + fw[spot, :] * far
        out[pl.ds(base * FIELD + j, count, stride=ROWS), :] = value

    complete(OZ)

    def ozone_row(j, carry):
        advect(j, oz, LEV, 7)
        return carry

    lax.fori_loop(0, ROWS, ozone_row, 0)

    def step(k, carry):
        @pl.when(k < NB)
        def _():
            forward(k)

        @pl.when(jnp.logical_and(k >= LAG_B, k < NB + LAG_B))
        def _():
            forward_relayed(k - LAG_B)

        @pl.when(k >= LAG_C)
        def _():
            complete(k - LAG_C)
            for r in range(CH):
                advect((k - LAG_C) * CH + r, qb, 4 * LEV, 3)

        return carry

    lax.fori_loop(0, NB + LAG_C, step, 0)

    all_edges(lambda copy: copy.wait_send())
    for ch in range(NCH):

        @pl.when(lat > 0)
        def _():
            row_copy(0, ch).wait_send()

        @pl.when(lat < N_LAT - 1)
        def _():
            row_copy(1, ch).wait_send()

    drain(OZ)

    def drain_block(n, carry):
        drain(n)
        return carry

    lax.fori_loop(0, NB, drain_block, 0)


def place(state, flux, state_out, flux_out, sem):
    copies = [pltpu.make_async_copy(flux, flux_out, sem.at[4])]
    for part in range(4):
        spot = slice(part * 2 * FIELD, (part + 1) * 2 * FIELD)
        copies.append(pltpu.make_async_copy(state.at[spot], state_out.at[spot], sem.at[part]))
    for copy in copies:
        copy.start()
    for copy in copies:
        copy.wait()


def on_device(state, surface, layer_one, layer_two, layer_three, layer_four, layer_five, lit_columns, row_offset):
    fields = state.shape[0]
    any_spec = pl.BlockSpec(memory_space=pl.ANY)
    vmem_spec = pl.BlockSpec(memory_space=pltpu.VMEM)
    dma = pltpu.SemaphoreType.DMA
    new_state, surface_flux = pl.pallas_call(
        kernel,
        out_shape=(
            pltpu.VMEM((fields * FIELD, COLS), F32),
            pltpu.VMEM((8 * ROWS, COLS), BF16),
        ),
        in_specs=[any_spec] * 8 + [pl.BlockSpec(memory_space=pltpu.SMEM)],
        out_specs=(vmem_spec, vmem_spec),
        scratch_shapes=[
            pltpu.VMEM((fields * FIELD, COLS), F32),
            pltpu.VMEM((76 * ROWS, COLS), BF16),
            pltpu.VMEM((76 * ROWS, COLS), F32),
            pltpu.VMEM((NIN, H1), BF16),
            pltpu.VMEM((H1, H2), BF16),
            pltpu.VMEM((H2, H3), BF16),
            pltpu.VMEM((H3, H4), BF16),
            pltpu.VMEM((NOUT, H4), BF16),
            pltpu.VMEM((ROWS, COLS), jnp.int32),
            pltpu.VMEM((ROWS * COLS, H1), F32),
            pltpu.VMEM((ROWS, COLS), F32),
            pltpu.VMEM((4 * FIELD, COLS), F32),
            pltpu.VMEM((4 * FIELD, COLS), F32),
            pltpu.VMEM((8 * ROWS, COLS), F32),
            pltpu.VMEM((FIELD, COLS), F32),
            pltpu.VMEM((2, NCH, LC * ROWS, COLS), BF16),
            pltpu.VMEM((2, NCH, LC * ROWS, COLS), BF16),
            pltpu.VMEM((EROWS, COLS), F32),
            pltpu.VMEM((EROWS, COLS), BF16),
            pltpu.VMEM((2, EROWS // 2, COLS), BF16),
            pltpu.VMEM((2, EROWS, COLS), BF16),
            pltpu.VMEM((6, EROWS // 2, COLS), BF16),
            pltpu.VMEM((10, GROUPS * ROWS, COLS), F32),
            pltpu.VMEM((5, ROWS, LEV, COLS), BF16),
            pltpu.VMEM((5, ROWS, 4 * LEV, COLS), BF16),
            dma((9,)),
            dma((2, NCH)),
            dma((2, NCH)),
            dma((8,)),
            dma((8,)),
            dma((NB + 1, 5)),
            dma((NB + 1, 5)),
        ],
        compiler_params=pltpu.CompilerParams(
            collective_id=0, has_side_effects=True, vmem_limit_bytes=56 * 1024 * 1024
        ),
    )(
        state.reshape(fields * FIELD, COLS),
        surface.reshape(76 * ROWS, COLS),
        layer_one, layer_two, layer_three, layer_four, layer_five.T,
        lit_columns.reshape(ROWS, COLS),
        row_offset,
    )
    new_state, surface_flux = pl.pallas_call(
        place,
        out_shape=(
            jax.ShapeDtypeStruct((fields * FIELD, COLS), F32),
            jax.ShapeDtypeStruct((8 * ROWS, COLS), BF16),
        ),
        in_specs=[vmem_spec, vmem_spec],
        out_specs=(any_spec, any_spec),
        scratch_shapes=[dma((5,))],
    )(pltpu.with_memory_space_constraint(new_state, pltpu.VMEM), pltpu.with_memory_space_constraint(surface_flux, pltpu.VMEM))
    return new_state.reshape(fields, LEV, ROWS, COLS), surface_flux.reshape(8, ROWS, COLS)


def solution(mesh):
    in_specs = (
        P(None, None, "lat", "lon"), P(None, "lat", "lon"), P(), P(), P(), P(), P(), P("lat", "lon", None), P("lat"),
    )
    out_specs = (P(None, None, "lat", "lon"), P(None, "lat", "lon"))
    return jax.shard_map(on_device, mesh=mesh, in_specs=in_specs, out_specs=out_specs, check_vma=False)
```

```python
import jax
import jax.numpy as jnp
from jax import lax
from jax.experimental import pallas as pl
from jax.experimental.pallas import tpu as pltpu
from jax.sharding import PartitionSpec as P

MESH = pl.DeviceIdType.MESH
F32, BF16 = jnp.float32, jnp.bfloat16

N_LAT, N_LON = 8, 16
LEV = 60
ROWS, COLS = 8, 128
FIELD = LEV * ROWS
COURANT = 0.6
STEP = 0.5
SLOPE = 0.15
DYN = 192
NIN, NOUT = 556, 368
H1, H2, H3, H4 = 768, 640, 512, 640

LC = 30
NCH = LEV // LC
PER = 15
GROUPS = LEV // PER
EROWS = 3 * GROUPS * ROWS
CH = 2
LAG_B, LAG_C = 1, 2
NB = ROWS // CH
OZ = NB

AROUND = ((0, -1), (0, 1), (-1, 0), (1, 0), (-1, -1), (-1, 1), (1, -1), (1, 1))
A1, B1, ZA, ZB, ZF = 0, 4, 7, 8, 9


def nt(a, b):
    return lax.dot_general(a, b, (((1,), (1,)), ((), ())), preferred_element_type=F32)


def eye(n):
    return (lax.broadcasted_iota(jnp.int32, (n, n), 0) == lax.broadcasted_iota(jnp.int32, (n, n), 1)).astype(F32).astype(BF16)


def leaky(z):
    return jnp.maximum(z, SLOPE * z).astype(BF16)


def kernel(
    state, surface, w1h, w2h, w3h, w4h, w5h, lith, off,
    out, flux,
    st, sfb, sf, w1, w2, w3, w4, w5t, lit, acc, mask, fr, fw, fl,
    own_div, rsend, rrecv, own_edge, esend, hsend, erecv, hrecv, give, oz, qb,
    load_sem, rs_sem, rr_sem, es_sem, er_sem, qs_sem, qr_sem,
):
    lat, lon = lax.axis_index("lat"), lax.axis_index("lon")
    core, quarter = lax.rem(lon, 2), lax.rem(lon, 4)

    def at(dlat, dlon):
        return (lat + dlat, lax.rem(lon + dlon + N_LON, N_LON))

    loads = [
        pltpu.make_async_copy(state.at[0 : 3 * FIELD], st.at[0 : 3 * FIELD], load_sem.at[0]),
        pltpu.make_async_copy(state.at[3 * FIELD : 8 * FIELD], st.at[3 * FIELD : 8 * FIELD], load_sem.at[1]),
        pltpu.make_async_copy(surface, sfb, load_sem.at[2]),
        pltpu.make_async_copy(lith, lit, load_sem.at[3]),
        pltpu.make_async_copy(w1h, w1, load_sem.at[4]),
        pltpu.make_async_copy(w5h, w5t, load_sem.at[5]),
        pltpu.make_async_copy(w2h, w2, load_sem.at[6]),
        pltpu.make_async_copy(w3h, w3, load_sem.at[7]),
        pltpu.make_async_copy(w4h, w4, load_sem.at[8]),
    ]
    for load in loads:
        load.start()

    barrier = pltpu.get_barrier_semaphore()

    def greet(dlat, dlon):
        pl.semaphore_signal(barrier, inc=1, device_id=at(dlat, dlon), device_id_type=MESH)

    for dlon in (-4, -3, -2, -1, 1, 2, 3, 4):
        greet(0, dlon)

    @pl.when(lat > 0)
    def _():
        for dlon in (-1, 0, 1):
            greet(-1, dlon)

    @pl.when(lat < N_LAT - 1)
    def _():
        for dlon in (-1, 0, 1):
            greet(1, dlon)

    loads[0].wait()
    shape = (LC, ROWS, COLS)
    lane = lax.broadcasted_iota(jnp.int32, shape, 2)
    sub = lax.broadcasted_iota(jnp.int32, shape, 1)
    for ch in range(NCH):
        z, m, p = (
            st[f * FIELD + ch * LC * ROWS : f * FIELD + (ch + 1) * LC * ROWS].reshape(shape) for f in range(3)
        )
        m = jnp.where(lat * ROWS + sub < N_LAT * ROWS - 1, m, 0.0)
        m_south = pltpu.roll(m, 1, 1)
        z_west = jnp.where(lane == 0, 0.0, pltpu.roll(z, 1, 2))
        d = COURANT * (z - z_west + m - jnp.where(sub == 0, 0.0, m_south))
        own_div[ch * LC * ROWS : (ch + 1) * LC * ROWS] = d.reshape(LC * ROWS, COLS)
        d_turned = pltpu.roll(d, 4, 1)
        to_south = jnp.where(sub < 4, p, d_turned)
        to_north = jnp.where(sub >= 4, p, jnp.where(sub >= 1, d_turned, m_south))
        rsend[0, ch] = to_south.reshape(LC * ROWS, COLS).astype(BF16)
        rsend[1, ch] = to_north.reshape(LC * ROWS, COLS).astype(BF16)
    lane2 = lax.broadcasted_iota(jnp.int32, (ROWS, COLS), 1)
    packed = []
    for f in range(3):
        for g in range(GROUPS):
            total = jnp.zeros((ROWS, COLS), F32)
            for kk in range(PER):
                row = (f * LEV + g * PER + kk) * ROWS
                total = jnp.where(lane2 // 8 == kk, pltpu.roll(st[row : row + ROWS], 4 + 8 * kk, 1), total)
            packed.append(total)
    own_edge[...] = jnp.concatenate(packed, axis=0)
    edges = own_edge[...]
    esend[...] = edges.astype(BF16)
    edges = edges.reshape(2, 3 * GROUPS // 2, ROWS, COLS)
    low, high = edges[0], edges[1]
    half = lax.broadcasted_iota(jnp.int32, low.shape, 1) < 4
    hsend[0] = jnp.where(half, low, pltpu.roll(high, 4, 1)).reshape(EROWS // 2, COLS).astype(BF16)
    hsend[1] = jnp.where(half, pltpu.roll(low, 4, 1), high).reshape(EROWS // 2, COLS).astype(BF16)

    neighbours = 8 + 3 * ((lat + N_LAT - 1) // N_LAT) + 3 * ((2 * N_LAT - 2 - lat) // N_LAT)
    pl.semaphore_wait(barrier, neighbours)

    def row_copy(side, ch):
        return pltpu.make_async_remote_copy(
            src_ref=rsend.at[side, ch], dst_ref=rrecv.at[side, ch],
            send_sem=rs_sem.at[side, ch], recv_sem=rr_sem.at[side, ch],
            device_id=at(2 * side - 1, 0), device_id_type=MESH,
        )

    def edge_copy(e):
        dlat, dlon = AROUND[e]
        place = AROUND.index((-dlat, -dlon))
        if dlat == 0:
            source, target = esend, erecv.at[place]
        else:
            source, target = hsend.at[(dlat + 1) // 2], hrecv.at[place - 2]
        return pltpu.make_async_remote_copy(
            src_ref=source, dst_ref=target,
            send_sem=es_sem.at[e], recv_sem=er_sem.at[place],
            device_id=at(dlat, dlon), device_id_type=MESH,
        )

    to_south, to_north = (2, 4, 5), (3, 6, 7)

    def all_edges(act):
        @pl.when(lat > 0)
        def _():
            for e in to_south:
                act(edge_copy(e))

        @pl.when(lat < N_LAT - 1)
        def _():
            for e in to_north:
                act(edge_copy(e))

        act(edge_copy(0))
        act(edge_copy(1))

    all_edges(lambda copy: copy.start())
    for ch in range(NCH):

        @pl.when(lat > 0)
        def _():
            row_copy(0, ch).start()

        @pl.when(lat < N_LAT - 1)
        def _():
            row_copy(1, ch).start()

    @pl.when(lat == 0)
    def _():
        rrecv[1] = jnp.zeros(rrecv.shape[1:], BF16)
        for e in to_south:
            hrecv[e - 2] = jnp.zeros(hrecv.shape[1:], BF16)

    @pl.when(lat == N_LAT - 1)
    def _():
        rrecv[0] = jnp.zeros(rrecv.shape[1:], BF16)
        for e in to_north:
            hrecv[e - 2] = jnp.zeros(hrecv.shape[1:], BF16)

    def block(n, slot):
        if isinstance(n, int) and n == OZ:
            return oz.at[slot]
        return qb.at[slot, pl.ds(n * CH, CH)]

    def send(n, flow, source, slot, dlon):
        return pltpu.make_async_remote_copy(
            src_ref=block(n, source), dst_ref=block(n, slot),
            send_sem=qs_sem.at[n, flow], recv_sem=qr_sem.at[n, slot],
            device_id=at(0, dlon), device_id_type=MESH,
        )

    def flow(name, n):
        if name == "y" or name == "d":
            return send(n, 0 if name == "d" else 1, 0, 2, 2)
        if name == "z":
            return send(n, 0, 0, 3, 3)
        if name == "x":
            return send(n, 0, 0, 4, 4)
        if name == "s":
            return send(n, 1, 4, 3, -1)
        if name == "e":
            return send(n, 3, 0, 2, 2)
        if name == "p":
            return send(n, 2, 0, 1, 1)
        if name == "r":
            return send(n, 3, 4, 2, -2)
        if name == "f":
            return send(n, 4, 2, 3, 1)
        return send(n, 4, 2, 1, -1)

    sources = {
        "y": quarter < 2, "d": quarter == 2, "z": quarter == 1, "x": quarter == 3, "p": core == 0,
        "r": quarter == 3, "e": quarter == 3, "s": quarter == 3, "f": core == 0, "g": quarter == 3, "h": quarter == 1,
    }
    drains = {
        "y": quarter >= 2, "d": quarter == 0, "z": quarter == 0, "x": quarter == 3, "p": core == 1,
        "r": quarter == 1, "s": quarter == 2, "f": core == 1, "g": quarter == 2, "h": quarter == 0,
    }

    def do(name, n, act):
        @pl.when(sources[name])
        def _():
            act(flow(name, n))

    def got(name, n):
        @pl.when(drains[name])
        def _():
            flow(name, n).wait_recv()

    def first_hops(n, act):
        for name in "xdyzp":
            do(name, n, act)

    def begin(copy):
        copy.start()

    def relayed(n, act):
        if isinstance(n, int):
            do("r", n, act)
        else:

            @pl.when(n > 0)
            def _():
                do("r", n, act)

    def straight(n, act):
        if not isinstance(n, int):

            @pl.when(n == 0)
            def _():
                do("e", n, act)

    def relay(n):
        got("x", n)
        relayed(n, begin)
        do("s", n, begin)

    def forward(n):
        got("d", n)
        got("y", n)
        do("f", n, begin)
        do("g", n, begin)

    def forward_relayed(n):
        got("r", n)
        do("h", n, begin)

    def complete(n):
        got("z", n)
        got("s", n)
        got("p", n)
        got("g", n)
        got("h", n)
        got("f", n)

    def drain(n):
        def sent(copy):
            copy.wait_send()

        for name in "ydzxpsfgh":
            do(name, n, sent)
        relayed(n, sent)
        straight(n, sent)

    loads[1].wait()
    for j in range(ROWS):
        oz[0, j] = st[pl.ds(7 * FIELD + j, LEV, stride=ROWS), :].astype(BF16)
    first_hops(OZ, lambda copy: copy.start())
    loads[2].wait()
    sf[...] = sfb[...].astype(F32)
    loads[3].wait()
    listed = lit[...]
    row_id = lax.broadcasted_iota(jnp.int32, (ROWS, COLS), 0)
    col_id = lax.broadcasted_iota(jnp.int32, (COLS, COLS), 0)
    in_row, in_col = [], []
    for r in range(ROWS):
        entry = listed[r : r + 1]
        in_row.append(jnp.where(jnp.broadcast_to(entry >> 7, (ROWS, COLS)) == row_id, 1.0, 0.0))
        in_col.append(jnp.where(jnp.broadcast_to(entry & 127, (COLS, COLS)) == col_id, 1.0, 0.0))
    mask[...] = nt(jnp.concatenate(in_row, 1).astype(BF16), jnp.concatenate(in_col, 1).astype(BF16))
    loads[4].wait()
    eye_c = eye(COLS)

    def static_rows(j, carry):
        tracers = st[pl.ds(DYN * ROWS + j, 8 * LEV - DYN, stride=ROWS), :]
        ground = sf[pl.ds(j, 76, stride=ROWS), :]
        x = jnp.concatenate([tracers, ground], axis=0).astype(BF16)
        xt = nt(eye_c, x).astype(BF16)
        spot = pl.ds(pl.multiple_of(j * COLS, COLS), COLS)
        acc[spot, :] = jnp.dot(xt, w1[DYN:NIN], preferred_element_type=F32)
        return carry

    lax.fori_loop(0, ROWS, static_rows, 0)
    loads[5].wait()

    def edge_arrival(place):
        dlat, dlon = AROUND[place]
        if dlat == 0:
            source, target = esend, erecv.at[place]
        else:
            source, target = hsend.at[0], hrecv.at[place - 2]
        return pltpu.make_async_remote_copy(
            src_ref=source, dst_ref=target, send_sem=es_sem.at[place], recv_sem=er_sem.at[place],
            device_id=at(dlat, dlon), device_id_type=MESH,
        )

    @pl.when(lat > 0)
    def _():
        for e in to_south:
            edge_arrival(e).wait_recv()

    @pl.when(lat < N_LAT - 1)
    def _():
        for e in to_north:
            edge_arrival(e).wait_recv()

    edge_arrival(0).wait_recv()
    edge_arrival(1).wait_recv()

    strip_shape = (2 * GROUPS, ROWS, COLS)
    s_lane = lax.broadcasted_iota(jnp.int32, strip_shape, 2) % 8
    s_sub = lax.broadcasted_iota(jnp.int32, strip_shape, 1)
    group_shape = (3 * GROUPS, ROWS, COLS)
    first_half = lax.broadcasted_iota(jnp.int32, group_shape, 2) % 8 < 4

    def opened(sub):
        row_a = lat * ROWS + sub
        row_b = lat * ROWS + jnp.where(sub < 4, sub + ROWS, sub - ROWS)
        return row_a < N_LAT * ROWS - 1, jnp.logical_and(row_b >= 0, row_b < N_LAT * ROWS - 1)

    def beyond(north_place, south_place):
        nn = hrecv[north_place - 2].astype(F32).reshape(half.shape)
        ss = hrecv[south_place - 2].astype(F32).reshape(half.shape)
        return jnp.concatenate(
            [jnp.where(half, nn, pltpu.roll(ss, 4, 1)), jnp.where(half, pltpu.roll(nn, 4, 1), ss)], axis=0
        )

    def strips(west_edge, middle, east_edge):
        on_east, on_west = jnp.where(first_half, middle, east_edge), jnp.where(first_half, west_edge, middle)
        return [
            jnp.concatenate([on_east[f * GROUPS : (f + 1) * GROUPS], on_west[f * GROUPS : (f + 1) * GROUPS]], axis=0)
            for f in range(3)
        ]

    za, ma, pa = strips(
        erecv[0].astype(F32).reshape(group_shape), own_edge[...].reshape(group_shape), erecv[1].astype(F32).reshape(group_shape)
    )
    zb, mb, pb = strips(beyond(6, 4), beyond(3, 2), beyond(7, 5))

    def turn(x, steps):
        return pltpu.roll(x, steps % COLS, 2)

    def north(sub, x, y):
        x, y = pltpu.roll(x, ROWS - 1, 1), pltpu.roll(y, ROWS - 1, 1)
        return jnp.where(sub == ROWS - 1, y, x), jnp.where(sub == ROWS - 1, x, y)

    def south(sub, x, y):
        x, y = pltpu.roll(x, 1, 1), pltpu.roll(y, 1, 1)
        return jnp.where(sub == 0, y, x), jnp.where(sub == 0, x, y)

    def hand(index, value):
        merged = jnp.where(s_lane[:GROUPS] == 2, turn(value[:GROUPS], -2), value[GROUPS:])
        give[index] = merged.reshape(GROUPS * ROWS, COLS)

    square = COURANT * COURANT
    open_a, open_b = opened(s_sub)
    ma, mb = jnp.where(open_a, ma, 0.0), jnp.where(open_b, mb, 0.0)
    msa, msb = south(s_sub, ma, mb)
    da = COURANT * (za - turn(za, 1) + ma - msa)
    db = COURANT * (zb - turn(zb, 1) + mb - msb)
    hand(ZA, COURANT * za)
    hand(ZB, COURANT * zb)
    sa, sb = pa, pb
    for step in range(4):
        hand(A1 + step, sa)
        if step < 3:
            hand(B1 + step, sb)
            na, nb = north(s_sub, sa, sb)
            ga, gb = jnp.where(open_a, na - sa, 0.0), jnp.where(open_b, nb - sb, 0.0)
            gsa, gsb = south(s_sub, ga, gb)
            pa = pa - da + square * (turn(sa, -1) + turn(sa, 1) - 2.0 * sa + ga - gsa)
            pb = pb - db + square * (turn(sb, -1) + turn(sb, 1) - 2.0 * sb + gb - gsb)
            sa, sb = sa + pa, sb + pb
    hand(ZF, za - COURANT * (turn(sa, -1) - sa))

    open_a, open_b = opened(sub)
    first_lane, last_lane = lane == 0, lane == COLS - 1

    def acoustic(ch, carry):
        @pl.when(lat > 0)
        def _():
            row_copy(1, ch).wait_recv()

        @pl.when(lat < N_LAT - 1)
        def _():
            row_copy(0, ch).wait_recv()

        def spot_of(f):
            return pl.ds(pl.multiple_of(f * FIELD + ch * LC * ROWS, ROWS), LC * ROWS)

        def given(index):
            pieces = []
            for g in range(LC // PER):
                group = give[index, pl.ds(pl.multiple_of((ch * (LC // PER) + g) * ROWS, ROWS), ROWS), :]
                for kk in range(PER):
                    pieces.append(pltpu.roll(group, (COLS - 3 - 8 * kk) % COLS, 1).reshape(1, ROWS, COLS))
            return jnp.concatenate(pieces, axis=0)

        def sides(x, other):
            return jnp.where(last_lane, other, turn(x, -1)) + jnp.where(first_lane, other, turn(x, 1))

        from_north = rrecv[0, ch].astype(F32).reshape(shape)
        from_south = rrecv[1, ch].astype(F32).reshape(shape)
        pb = jnp.where(sub < 4, from_north, from_south)
        db = pltpu.roll(jnp.where(sub < 4, from_south, from_north), 4, 1)
        ma = jnp.where(open_a, st[spot_of(1), :].reshape(shape), 0.0)
        db = db - jnp.where(first_lane, given(ZB), 0.0) - jnp.where(sub == 0, COURANT * pltpu.roll(ma, 1, 1), 0.0)
        da = own_div[spot_of(0), :].reshape(shape)
        da = da - jnp.where(first_lane, given(ZA), 0.0) - jnp.where(sub == 0, COURANT * from_south, 0.0)
        pa = st[spot_of(2), :].reshape(shape)
        sa, sb = pa, pb
        for step in range(4):
            na, nb = north(sub, sa, sb)
            ga, gb = jnp.where(open_a, na - sa, 0.0), jnp.where(open_b, nb - sb, 0.0)
            gsa, gsb = south(sub, ga, gb)
            other = given(A1 + step)
            if step == 3:
                ea = jnp.where(last_lane, other, turn(sa, -1))
                across = ea + jnp.where(first_lane, other, turn(sa, 1))
            else:
                across = sides(sa, other)
            pa = pa - da + square * (across - 2.0 * sa + ga - gsa)
            if step < 3:
                pb = pb - db + square * (sides(sb, given(B1 + step)) - 2.0 * sb + gb - gsb)
                sa, sb = sa + pa, sb + pb
        za = st[spot_of(0), :].reshape(shape) - COURANT * (ea - sa)
        ma = jnp.where(open_a, ma - COURANT * ga, 0.0)
        z_west = jnp.where(first_lane, given(ZF), turn(za, 1))
        share = (0.5 + 0.45 * jnp.tanh(za)).reshape(LC * ROWS, COLS)
        share_west = (0.5 + 0.45 * jnp.tanh(z_west)).reshape(LC * ROWS, COLS)
        for f, value in enumerate((za, ma, pa)):
            st[spot_of(f), :] = value.reshape(LC * ROWS, COLS)
        out[spot_of(2), :] = pa.reshape(LC * ROWS, COLS)
        for f in range(4):
            fr[spot_of(f), :] = share
            fw[spot_of(f), :] = share_west
        return carry

    lax.fori_loop(0, NCH, acoustic, 0)

    relay(OZ)
    forward(OZ)
    for load in loads[6:]:
        load.wait()

    def network(n, carry):
        xs = []
        for r in range(CH):
            x = st[pl.ds(n * CH + r, DYN, stride=ROWS), :].astype(BF16)
            xs.append(nt(eye_c, x).astype(BF16))
        xt = jnp.concatenate(xs, axis=0)
        spot = pl.ds(pl.multiple_of(n * CH * COLS, COLS), CH * COLS)
        h = leaky(acc[spot, :] + jnp.dot(xt, w1[0:DYN], preferred_element_type=F32))
        for w in (w2, w3, w4):
            h = leaky(jnp.dot(h, w[...], preferred_element_type=F32))
        y = nt(w5t[...], h)
        for r in range(CH):
            j = n * CH + r
            t = jnp.where(jnp.broadcast_to(mask[pl.ds(j, 1), :], (NOUT, COLS)) > 0.5, y[:, r * COLS : (r + 1) * COLS], 0.0)
            q = st[pl.ds(3 * FIELD + j, 4 * LEV, stride=ROWS), :] + STEP * t[2 * LEV : 6 * LEV]
            qb[0, j] = q.astype(BF16)
            out[pl.ds(j, 2 * LEV, stride=ROWS), :] = st[pl.ds(j, 2 * LEV, stride=ROWS), :] + STEP * t[0 : 2 * LEV]
            fl[pl.ds(j, 8, stride=ROWS), :] = t[6 * LEV :]
        first_hops(n, begin)
        straight(n, begin)
        return carry

    lax.fori_loop(0, ROWS // CH, network, 0)
    forward_relayed(OZ)

    @pl.when(quarter == 3)
    def _():
        def relay_row(n, carry):
            relay(n)
            return carry

        lax.fori_loop(0, NB, relay_row, 0)

    flux[...] = fl[...].astype(BF16)

    def advect(j, ref, count, base):
        offset = off[j]
        tiles, cells = offset >> 7, offset & 127
        tile_shape = (count, COLS)
        where = lax.broadcasted_iota(jnp.int32, tile_shape, 1)
        parts = [ref[slot, j].astype(F32) for slot in range(4)]

        def pick(cut):
            d = tiles + jnp.where(where >= cut, 1, 0)
            return jnp.where(d == 0, parts[0], jnp.where(d == 1, parts[1], jnp.where(d == 2, parts[2], parts[3])))

        near = pltpu.roll(pick(COLS - cells), cells, 1)
        far = pltpu.roll(pick(COLS - 1 - cells), (cells + 1) & 127, 1)
        spot = pl.ds(j, count, stride=ROWS)
        value = (1.0 - fr[spot, :]) * near + fw[spot, :] * far
        out[pl.ds(base * FIELD + j, count, stride=ROWS), :] = value

    complete(OZ)

    def ozone_row(j, carry):
        advect(j, oz, LEV, 7)
        return carry

    lax.fori_loop(0, ROWS, ozone_row, 0)

    def step(k, carry):
        @pl.when(k < NB)
        def _():
            forward(k)

        @pl.when(jnp.logical_and(k >= LAG_B, k < NB + LAG_B))
        def _():
            forward_relayed(k - LAG_B)

        @pl.when(k >= LAG_C)
        def _():
            complete(k - LAG_C)
            for r in range(CH):
                advect((k - LAG_C) * CH + r, qb, 4 * LEV, 3)

        return carry

    lax.fori_loop(0, NB + LAG_C, step, 0)

    all_edges(lambda copy: copy.wait_send())
    for ch in range(NCH):

        @pl.when(lat > 0)
        def _():
            row_copy(0, ch).wait_send()

        @pl.when(lat < N_LAT - 1)
        def _():
            row_copy(1, ch).wait_send()

    drain(OZ)

    def drain_block(n, carry):
        drain(n)
        return carry

    lax.fori_loop(0, NB, drain_block, 0)


def place(state, flux, state_out, flux_out, sem):
    copies = [pltpu.make_async_copy(flux, flux_out, sem.at[4])]
    for part in range(4):
        spot = slice(part * 2 * FIELD, (part + 1) * 2 * FIELD)
        copies.append(pltpu.make_async_copy(state.at[spot], state_out.at[spot], sem.at[part]))
    for copy in copies:
        copy.start()
    for copy in copies:
        copy.wait()


def on_device(state, surface, layer_one, layer_two, layer_three, layer_four, layer_five, lit_columns, row_offset):
    fields = state.shape[0]
    any_spec = pl.BlockSpec(memory_space=pl.ANY)
    vmem_spec = pl.BlockSpec(memory_space=pltpu.VMEM)
    dma = pltpu.SemaphoreType.DMA
    new_state, surface_flux = pl.pallas_call(
        kernel,
        out_shape=(
            pltpu.VMEM((fields * FIELD, COLS), F32),
            pltpu.VMEM((8 * ROWS, COLS), BF16),
        ),
        in_specs=[any_spec] * 8 + [pl.BlockSpec(memory_space=pltpu.SMEM)],
        out_specs=(vmem_spec, vmem_spec),
        scratch_shapes=[
            pltpu.VMEM((fields * FIELD, COLS), F32),
            pltpu.VMEM((76 * ROWS, COLS), BF16),
            pltpu.VMEM((76 * ROWS, COLS), F32),
            pltpu.VMEM((NIN, H1), BF16),
            pltpu.VMEM((H1, H2), BF16),
            pltpu.VMEM((H2, H3), BF16),
            pltpu.VMEM((H3, H4), BF16),
            pltpu.VMEM((NOUT, H4), BF16),
            pltpu.VMEM((ROWS, COLS), jnp.int32),
            pltpu.VMEM((ROWS * COLS, H1), F32),
            pltpu.VMEM((ROWS, COLS), F32),
            pltpu.VMEM((4 * FIELD, COLS), F32),
            pltpu.VMEM((4 * FIELD, COLS), F32),
            pltpu.VMEM((8 * ROWS, COLS), F32),
            pltpu.VMEM((FIELD, COLS), F32),
            pltpu.VMEM((2, NCH, LC * ROWS, COLS), BF16),
            pltpu.VMEM((2, NCH, LC * ROWS, COLS), BF16),
            pltpu.VMEM((EROWS, COLS), F32),
            pltpu.VMEM((EROWS, COLS), BF16),
            pltpu.VMEM((2, EROWS // 2, COLS), BF16),
            pltpu.VMEM((2, EROWS, COLS), BF16),
            pltpu.VMEM((6, EROWS // 2, COLS), BF16),
            pltpu.VMEM((10, GROUPS * ROWS, COLS), F32),
            pltpu.VMEM((5, ROWS, LEV, COLS), BF16),
            pltpu.VMEM((5, ROWS, 4 * LEV, COLS), BF16),
            dma((9,)),
            dma((2, NCH)),
            dma((2, NCH)),
            dma((8,)),
            dma((8,)),
            dma((NB + 1, 5)),
            dma((NB + 1, 5)),
        ],
        compiler_params=pltpu.CompilerParams(
            collective_id=0, has_side_effects=True, vmem_limit_bytes=56 * 1024 * 1024
        ),
    )(
        state.reshape(fields * FIELD, COLS),
        surface.reshape(76 * ROWS, COLS),
        layer_one, layer_two, layer_three, layer_four, layer_five.T,
        lit_columns.reshape(ROWS, COLS),
        row_offset,
    )
    new_state, surface_flux = pl.pallas_call(
        place,
        out_shape=(
            jax.ShapeDtypeStruct((fields * FIELD, COLS), F32),
            jax.ShapeDtypeStruct((8 * ROWS, COLS), BF16),
        ),
        in_specs=[vmem_spec, vmem_spec],
        out_specs=(any_spec, any_spec),
        scratch_shapes=[dma((5,))],
    )(pltpu.with_memory_space_constraint(new_state, pltpu.VMEM), pltpu.with_memory_space_constraint(surface_flux, pltpu.VMEM))
    return new_state.reshape(fields, LEV, ROWS, COLS), surface_flux.reshape(8, ROWS, COLS)


def solution(mesh):
    in_specs = (
        P(None, None, "lat", "lon"), P(None, "lat", "lon"), P(), P(), P(), P(), P(), P("lat", "lon", None), P("lat"),
    )
    out_specs = (P(None, None, "lat", "lon"), P(None, "lat", "lon"))
    return jax.shard_map(on_device, mesh=mesh, in_specs=in_specs, out_specs=out_specs, check_vma=False)
```

```python
import jax
import jax.numpy as jnp
from jax import lax
from jax.experimental import pallas as pl
from jax.experimental.pallas import tpu as pltpu
from jax.sharding import PartitionSpec as P

MESH = pl.DeviceIdType.MESH
F32, BF16 = jnp.float32, jnp.bfloat16

N_LAT, N_LON = 8, 16
LEV = 60
ROWS, COLS = 8, 128
FIELD = LEV * ROWS
COURANT = 0.6
STEP = 0.5
SLOPE = 0.15
SPARE = 64
DYN = 192
NIN, NOUT = 556, 368
H1, H2, H3, H4 = 768, 640, 512, 640

LC = 30
NCH = LEV // LC
PER = 15
GROUPS = LEV // PER
EROWS = 3 * GROUPS * ROWS
CH = 2
LAG_B, LAG_C = 1, 2
NB = ROWS // CH
OZ = NB

AROUND = ((0, -1), (0, 1), (-1, 0), (1, 0), (-1, -1), (-1, 1), (1, -1), (1, 1))
A1, B1, ZA, ZB, ZF = 0, 4, 7, 8, 9


def nt(a, b):
    return lax.dot_general(a, b, (((1,), (1,)), ((), ())), preferred_element_type=F32)


def eye(n):
    return (lax.broadcasted_iota(jnp.int32, (n, n), 0) == lax.broadcasted_iota(jnp.int32, (n, n), 1)).astype(F32).astype(BF16)


def leaky(z):
    return jnp.maximum(z, SLOPE * z).astype(BF16)


def kernel(
    state, surface, w1h, w2h, w3h, w4h, w5h, lith, off,
    out, flux,
    st, sfb, sf, w1, w2, w3, w4, w5t, lit, acc, mask, fr, fw, fl,
    own_div, rsend, rrecv, own_edge, esend, hsend, erecv, hrecv, give, oz, qb,
    load_sem, rs_sem, rr_sem, es_sem, er_sem, qs_sem, qr_sem,
):
    lat, lon = lax.axis_index("lat"), lax.axis_index("lon")
    core, quarter = lax.rem(lon, 2), lax.rem(lon, 4)

    def at(dlat, dlon):
        return (lat + dlat, lax.rem(lon + dlon + N_LON, N_LON))

    loads = [
        pltpu.make_async_copy(state.at[0 : 3 * FIELD], st.at[0 : 3 * FIELD], load_sem.at[0]),
        pltpu.make_async_copy(state.at[3 * FIELD : 8 * FIELD], st.at[3 * FIELD : 8 * FIELD], load_sem.at[1]),
        pltpu.make_async_copy(surface, sfb, load_sem.at[2]),
        pltpu.make_async_copy(lith, lit, load_sem.at[3]),
        pltpu.make_async_copy(w1h, w1, load_sem.at[4]),
        pltpu.make_async_copy(w5h, w5t, load_sem.at[5]),
        pltpu.make_async_copy(w2h, w2, load_sem.at[6]),
        pltpu.make_async_copy(w3h, w3, load_sem.at[7]),
        pltpu.make_async_copy(w4h, w4, load_sem.at[8]),
    ]
    for load in loads:
        load.start()

    barrier = pltpu.get_barrier_semaphore()

    def greet(dlat, dlon):
        pl.semaphore_signal(barrier, inc=1, device_id=at(dlat, dlon), device_id_type=MESH)

    for dlon in (-4, -3, -2, -1, 1, 2, 3, 4):
        greet(0, dlon)

    @pl.when(lat > 0)
    def _():
        for dlon in (-1, 0, 1):
            greet(-1, dlon)

    @pl.when(lat < N_LAT - 1)
    def _():
        for dlon in (-1, 0, 1):
            greet(1, dlon)

    loads[0].wait()
    shape = (LC, ROWS, COLS)
    lane = lax.broadcasted_iota(jnp.int32, shape, 2)
    sub = lax.broadcasted_iota(jnp.int32, shape, 1)
    for ch in range(NCH):
        z, m, p = (
            st[f * FIELD + ch * LC * ROWS : f * FIELD + (ch + 1) * LC * ROWS].reshape(shape) for f in range(3)
        )
        m = jnp.where(lat * ROWS + sub < N_LAT * ROWS - 1, m, 0.0)
        m_south = pltpu.roll(m, 1, 1)
        z_west = jnp.where(lane == 0, 0.0, pltpu.roll(z, 1, 2))
        d = COURANT * (z - z_west + m - jnp.where(sub == 0, 0.0, m_south))
        own_div[ch * LC * ROWS : (ch + 1) * LC * ROWS] = d.reshape(LC * ROWS, COLS)
        d_turned = pltpu.roll(d, 4, 1)
        to_south = jnp.where(sub < 4, p, d_turned)
        to_north = jnp.where(sub >= 4, p, jnp.where(sub >= 1, d_turned, m_south))
        rsend[0, ch] = to_south.reshape(LC * ROWS, COLS).astype(BF16)
        rsend[1, ch] = to_north.reshape(LC * ROWS, COLS).astype(BF16)
    lane2 = lax.broadcasted_iota(jnp.int32, (ROWS, COLS), 1)
    packed = []
    for f in range(3):
        for g in range(GROUPS):
            total = jnp.zeros((ROWS, COLS), F32)
            for kk in range(PER):
                row = (f * LEV + g * PER + kk) * ROWS
                total = jnp.where(lane2 // 8 == kk, pltpu.roll(st[row : row + ROWS], 4 + 8 * kk, 1), total)
            packed.append(total)
    own_edge[...] = jnp.concatenate(packed, axis=0)
    edges = own_edge[...]
    esend[...] = edges.astype(BF16)
    edges = edges.reshape(2, 3 * GROUPS // 2, ROWS, COLS)
    low, high = edges[0], edges[1]
    half = lax.broadcasted_iota(jnp.int32, low.shape, 1) < 4
    hsend[0] = jnp.where(half, low, pltpu.roll(high, 4, 1)).reshape(EROWS // 2, COLS).astype(BF16)
    hsend[1] = jnp.where(half, pltpu.roll(low, 4, 1), high).reshape(EROWS // 2, COLS).astype(BF16)

    neighbours = 8 + 3 * ((lat + N_LAT - 1) // N_LAT) + 3 * ((2 * N_LAT - 2 - lat) // N_LAT)
    pl.semaphore_wait(barrier, neighbours)

    def row_copy(side, ch):
        return pltpu.make_async_remote_copy(
            src_ref=rsend.at[side, ch], dst_ref=rrecv.at[side, ch],
            send_sem=rs_sem.at[side, ch], recv_sem=rr_sem.at[side, ch],
            device_id=at(2 * side - 1, 0), device_id_type=MESH,
        )

    def edge_copy(e):
        dlat, dlon = AROUND[e]
        place = AROUND.index((-dlat, -dlon))
        if dlat == 0:
            source, target = esend, erecv.at[place]
        else:
            source, target = hsend.at[(dlat + 1) // 2], hrecv.at[place - 2]
        return pltpu.make_async_remote_copy(
            src_ref=source, dst_ref=target,
            send_sem=es_sem.at[e], recv_sem=er_sem.at[place],
            device_id=at(dlat, dlon), device_id_type=MESH,
        )

    to_south, to_north = (2, 4, 5), (3, 6, 7)

    def all_edges(act):
        @pl.when(lat > 0)
        def _():
            for e in to_south:
                act(edge_copy(e))

        @pl.when(lat < N_LAT - 1)
        def _():
            for e in to_north:
                act(edge_copy(e))

        act(edge_copy(0))
        act(edge_copy(1))

    all_edges(lambda copy: copy.start())
    for ch in range(NCH):

        @pl.when(lat > 0)
        def _():
            row_copy(0, ch).start()

        @pl.when(lat < N_LAT - 1)
        def _():
            row_copy(1, ch).start()

    @pl.when(lat == 0)
    def _():
        rrecv[1] = jnp.zeros(rrecv.shape[1:], BF16)
        for e in to_south:
            hrecv[e - 2] = jnp.zeros(hrecv.shape[1:], BF16)

    @pl.when(lat == N_LAT - 1)
    def _():
        rrecv[0] = jnp.zeros(rrecv.shape[1:], BF16)
        for e in to_north:
            hrecv[e - 2] = jnp.zeros(hrecv.shape[1:], BF16)

    def block(n, slot):
        if isinstance(n, int) and n == OZ:
            return oz.at[slot]
        return qb.at[slot, pl.ds(n * CH, CH)]

    def send(n, flow, source, slot, dlon):
        return pltpu.make_async_remote_copy(
            src_ref=block(n, source), dst_ref=block(n, slot),
            send_sem=qs_sem.at[n, flow], recv_sem=qr_sem.at[n, slot],
            device_id=at(0, dlon), device_id_type=MESH,
        )

    def flow(name, n):
        if name == "y" or name == "d":
            return send(n, 0 if name == "d" else 1, 0, 2, 2)
        if name == "z":
            return send(n, 0, 0, 3, 3)
        if name == "x":
            return send(n, 0, 0, 4, 4)
        if name == "s":
            return send(n, 1, 4, 3, -1)
        if name == "e":
            return send(n, 3, 0, 2, 2)
        if name == "p":
            return send(n, 2, 0, 1, 1)
        if name == "r":
            return send(n, 3, 4, 2, -2)
        if name == "f":
            return send(n, 4, 2, 3, 1)
        return send(n, 4, 2, 1, -1)

    sources = {
        "y": quarter < 2, "d": quarter == 2, "z": quarter == 1, "x": quarter == 3, "p": core == 0,
        "r": quarter == 3, "e": quarter == 3, "s": quarter == 3, "f": core == 0, "g": quarter == 3, "h": quarter == 1,
    }
    drains = {
        "y": quarter >= 2, "d": quarter == 0, "z": quarter == 0, "x": quarter == 3, "p": core == 1,
        "r": quarter == 1, "s": quarter == 2, "f": core == 1, "g": quarter == 2, "h": quarter == 0,
    }

    def do(name, n, act):
        @pl.when(sources[name])
        def _():
            act(flow(name, n))

    def got(name, n):
        @pl.when(drains[name])
        def _():
            flow(name, n).wait_recv()

    def first_hops(n, act):
        for name in "xdyzp":
            do(name, n, act)

    def begin(copy):
        copy.start()

    def relayed(n, act):
        if isinstance(n, int):
            do("r", n, act)
        else:

            @pl.when(n > 0)
            def _():
                do("r", n, act)

    def straight(n, act):
        if not isinstance(n, int):

            @pl.when(n == 0)
            def _():
                do("e", n, act)

    def relay(n):
        got("x", n)
        relayed(n, begin)
        do("s", n, begin)

    def forward(n):
        got("d", n)
        got("y", n)
        do("f", n, begin)
        do("g", n, begin)

    def forward_relayed(n):
        got("r", n)
        do("h", n, begin)

    def complete(n):
        got("z", n)
        got("s", n)
        got("p", n)
        got("g", n)
        got("h", n)
        got("f", n)

    def drain(n):
        def sent(copy):
            copy.wait_send()

        for name in "ydzxpsfgh":
            do(name, n, sent)
        relayed(n, sent)
        straight(n, sent)

    loads[1].wait()
    for j in range(ROWS):
        oz[0, j] = st[pl.ds(7 * FIELD + j, LEV, stride=ROWS), :].astype(BF16)
    first_hops(OZ, lambda copy: copy.start())
    loads[2].wait()
    sf[0 : 76 * ROWS] = sfb[...].astype(F32)
    loads[3].wait()
    listed = lit[...]
    row_id = lax.broadcasted_iota(jnp.int32, (ROWS, COLS), 0)
    col_id = lax.broadcasted_iota(jnp.int32, (COLS, COLS), 0)
    in_row, in_col = [], []
    for r in range(ROWS):
        entry = listed[r : r + 1]
        in_row.append(jnp.where(jnp.broadcast_to(entry >> 7, (ROWS, COLS)) == row_id, 1.0, 0.0))
        in_col.append(jnp.where(jnp.broadcast_to(entry & 127, (COLS, COLS)) == col_id, 1.0, 0.0))
    mask[0:ROWS] = nt(jnp.concatenate(in_row, 1).astype(BF16), jnp.concatenate(in_col, 1).astype(BF16))
    loads[4].wait()
    eye_c = eye(COLS)

    def static_rows(j, carry):
        tracers = st[pl.ds(DYN * ROWS + j, 8 * LEV - DYN, stride=ROWS), :]
        ground = sf[pl.ds(j, 76, stride=ROWS), :]
        x = jnp.concatenate([tracers, ground], axis=0).astype(BF16)
        xt = nt(eye_c, x).astype(BF16)
        spot = pl.ds(pl.multiple_of(j * COLS, COLS), COLS)
        acc[spot, :] = jnp.dot(xt, w1[DYN:NIN], preferred_element_type=F32)
        return carry

    lax.fori_loop(0, ROWS, static_rows, 0)
    loads[5].wait()

    def edge_arrival(place):
        dlat, dlon = AROUND[place]
        if dlat == 0:
            source, target = esend, erecv.at[place]
        else:
            source, target = hsend.at[0], hrecv.at[place - 2]
        return pltpu.make_async_remote_copy(
            src_ref=source, dst_ref=target, send_sem=es_sem.at[place], recv_sem=er_sem.at[place],
            device_id=at(dlat, dlon), device_id_type=MESH,
        )

    @pl.when(lat > 0)
    def _():
        for e in to_south:
            edge_arrival(e).wait_recv()

    @pl.when(lat < N_LAT - 1)
    def _():
        for e in to_north:
            edge_arrival(e).wait_recv()

    edge_arrival(0).wait_recv()
    edge_arrival(1).wait_recv()

    strip_shape = (2 * GROUPS, ROWS, COLS)
    s_lane = lax.broadcasted_iota(jnp.int32, strip_shape, 2) % 8
    s_sub = lax.broadcasted_iota(jnp.int32, strip_shape, 1)
    group_shape = (3 * GROUPS, ROWS, COLS)
    first_half = lax.broadcasted_iota(jnp.int32, group_shape, 2) % 8 < 4

    def opened(sub):
        row_a = lat * ROWS + sub
        row_b = lat * ROWS + jnp.where(sub < 4, sub + ROWS, sub - ROWS)
        return row_a < N_LAT * ROWS - 1, jnp.logical_and(row_b >= 0, row_b < N_LAT * ROWS - 1)

    def beyond(north_place, south_place):
        nn = hrecv[north_place - 2].astype(F32).reshape(half.shape)
        ss = hrecv[south_place - 2].astype(F32).reshape(half.shape)
        return jnp.concatenate(
            [jnp.where(half, nn, pltpu.roll(ss, 4, 1)), jnp.where(half, pltpu.roll(nn, 4, 1), ss)], axis=0
        )

    def strips(west_edge, middle, east_edge):
        on_east, on_west = jnp.where(first_half, middle, east_edge), jnp.where(first_half, west_edge, middle)
        return [
            jnp.concatenate([on_east[f * GROUPS : (f + 1) * GROUPS], on_west[f * GROUPS : (f + 1) * GROUPS]], axis=0)
            for f in range(3)
        ]

    za, ma, pa = strips(
        erecv[0].astype(F32).reshape(group_shape), own_edge[...].reshape(group_shape), erecv[1].astype(F32).reshape(group_shape)
    )
    zb, mb, pb = strips(beyond(6, 4), beyond(3, 2), beyond(7, 5))

    def turn(x, steps):
        return pltpu.roll(x, steps % COLS, 2)

    def north(sub, x, y):
        x, y = pltpu.roll(x, ROWS - 1, 1), pltpu.roll(y, ROWS - 1, 1)
        return jnp.where(sub == ROWS - 1, y, x), jnp.where(sub == ROWS - 1, x, y)

    def south(sub, x, y):
        x, y = pltpu.roll(x, 1, 1), pltpu.roll(y, 1, 1)
        return jnp.where(sub == 0, y, x), jnp.where(sub == 0, x, y)

    def hand(index, value):
        merged = jnp.where(s_lane[:GROUPS] == 2, turn(value[:GROUPS], -2), value[GROUPS:])
        give[index] = merged.reshape(GROUPS * ROWS, COLS)

    square = COURANT * COURANT
    open_a, open_b = opened(s_sub)
    ma, mb = jnp.where(open_a, ma, 0.0), jnp.where(open_b, mb, 0.0)
    msa, msb = south(s_sub, ma, mb)
    da = COURANT * (za - turn(za, 1) + ma - msa)
    db = COURANT * (zb - turn(zb, 1) + mb - msb)
    hand(ZA, COURANT * za)
    hand(ZB, COURANT * zb)
    sa, sb = pa, pb
    for step in range(4):
        hand(A1 + step, sa)
        if step < 3:
            hand(B1 + step, sb)
            na, nb = north(s_sub, sa, sb)
            ga, gb = jnp.where(open_a, na - sa, 0.0), jnp.where(open_b, nb - sb, 0.0)
            gsa, gsb = south(s_sub, ga, gb)
            pa = pa - da + square * (turn(sa, -1) + turn(sa, 1) - 2.0 * sa + ga - gsa)
            pb = pb - db + square * (turn(sb, -1) + turn(sb, 1) - 2.0 * sb + gb - gsb)
            sa, sb = sa + pa, sb + pb
    hand(ZF, za - COURANT * (turn(sa, -1) - sa))

    open_a, open_b = opened(sub)
    first_lane, last_lane = lane == 0, lane == COLS - 1

    def acoustic(ch, carry):
        @pl.when(lat > 0)
        def _():
            row_copy(1, ch).wait_recv()

        @pl.when(lat < N_LAT - 1)
        def _():
            row_copy(0, ch).wait_recv()

        def spot_of(f):
            return pl.ds(pl.multiple_of(f * FIELD + ch * LC * ROWS, ROWS), LC * ROWS)

        def given(index):
            pieces = []
            for g in range(LC // PER):
                group = give[index, pl.ds(pl.multiple_of((ch * (LC // PER) + g) * ROWS, ROWS), ROWS), :]
                for kk in range(PER):
                    pieces.append(pltpu.roll(group, (COLS - 3 - 8 * kk) % COLS, 1).reshape(1, ROWS, COLS))
            return jnp.concatenate(pieces, axis=0)

        def sides(x, other):
            return jnp.where(last_lane, other, turn(x, -1)) + jnp.where(first_lane, other, turn(x, 1))

        from_north = rrecv[0, ch].astype(F32).reshape(shape)
        from_south = rrecv[1, ch].astype(F32).reshape(shape)
        pb = jnp.where(sub < 4, from_north, from_south)
        db = pltpu.roll(jnp.where(sub < 4, from_south, from_north), 4, 1)
        ma = jnp.where(open_a, st[spot_of(1), :].reshape(shape), 0.0)
        db = db - jnp.where(first_lane, given(ZB), 0.0) - jnp.where(sub == 0, COURANT * pltpu.roll(ma, 1, 1), 0.0)
        da = own_div[spot_of(0), :].reshape(shape)
        da = da - jnp.where(first_lane, given(ZA), 0.0) - jnp.where(sub == 0, COURANT * from_south, 0.0)
        pa = st[spot_of(2), :].reshape(shape)
        sa, sb = pa, pb
        for step in range(4):
            na, nb = north(sub, sa, sb)
            ga, gb = jnp.where(open_a, na - sa, 0.0), jnp.where(open_b, nb - sb, 0.0)
            gsa, gsb = south(sub, ga, gb)
            other = given(A1 + step)
            if step == 3:
                ea = jnp.where(last_lane, other, turn(sa, -1))
                across = ea + jnp.where(first_lane, other, turn(sa, 1))
            else:
                across = sides(sa, other)
            pa = pa - da + square * (across - 2.0 * sa + ga - gsa)
            if step < 3:
                pb = pb - db + square * (sides(sb, given(B1 + step)) - 2.0 * sb + gb - gsb)
                sa, sb = sa + pa, sb + pb
        za = st[spot_of(0), :].reshape(shape) - COURANT * (ea - sa)
        ma = jnp.where(open_a, ma - COURANT * ga, 0.0)
        z_west = jnp.where(first_lane, given(ZF), turn(za, 1))
        share = (0.5 + 0.45 * jnp.tanh(za)).reshape(LC * ROWS, COLS)
        share_west = (0.5 + 0.45 * jnp.tanh(z_west)).reshape(LC * ROWS, COLS)
        for f, value in enumerate((za, ma, pa)):
            st[spot_of(f), :] = value.reshape(LC * ROWS, COLS)
        out[spot_of(2), :] = pa.reshape(LC * ROWS, COLS)
        for f in range(4):
            fr[spot_of(f), :] = share
            fw[spot_of(f), :] = share_west
        return carry

    lax.fori_loop(0, NCH, acoustic, 0)

    relay(OZ)
    forward(OZ)
    for load in loads[6:]:
        load.wait()

    def network(n, carry):
        xs = []
        for r in range(CH):
            x = st[pl.ds(n * CH + r, DYN, stride=ROWS), :].astype(BF16)
            xs.append(nt(eye_c, x).astype(BF16))
        xt = jnp.concatenate(xs, axis=0)
        spot = pl.ds(pl.multiple_of(n * CH * COLS, COLS), CH * COLS)
        h = leaky(acc[spot, :] + jnp.dot(xt, w1[0:DYN], preferred_element_type=F32))
        for w in (w2, w3, w4):
            h = leaky(jnp.dot(h, w[...], preferred_element_type=F32))
        y = nt(w5t[...], h)
        for r in range(CH):
            j = n * CH + r
            t = jnp.where(jnp.broadcast_to(mask[pl.ds(j, 1), :], (NOUT, COLS)) > 0.5, y[:, r * COLS : (r + 1) * COLS], 0.0)
            q = st[pl.ds(3 * FIELD + j, 4 * LEV, stride=ROWS), :] + STEP * t[2 * LEV : 6 * LEV]
            qb[0, j] = q.astype(BF16)
            out[pl.ds(j, 2 * LEV, stride=ROWS), :] = st[pl.ds(j, 2 * LEV, stride=ROWS), :] + STEP * t[0 : 2 * LEV]
            fl[pl.ds(j, 8, stride=ROWS), :] = t[6 * LEV :]
        first_hops(n, begin)
        straight(n, begin)
        return carry

    lax.fori_loop(0, ROWS // CH, network, 0)
    forward_relayed(OZ)

    @pl.when(quarter == 3)
    def _():
        def relay_row(n, carry):
            relay(n)
            return carry

        lax.fori_loop(0, NB, relay_row, 0)

    flux[...] = fl[...].astype(BF16)

    def advect(j, ref, count, base):
        offset = off[j]
        tiles, cells = offset >> 7, offset & 127
        tile_shape = (count, COLS)
        where = lax.broadcasted_iota(jnp.int32, tile_shape, 1)
        parts = [ref[slot, j].astype(F32) for slot in range(4)]

        def pick(cut):
            d = tiles + jnp.where(where >= cut, 1, 0)
            return jnp.where(d == 0, parts[0], jnp.where(d == 1, parts[1], jnp.where(d == 2, parts[2], parts[3])))

        near = pltpu.roll(pick(COLS - cells), cells, 1)
        far = pltpu.roll(pick(COLS - 1 - cells), (cells + 1) & 127, 1)
        spot = pl.ds(j, count, stride=ROWS)
        value = (1.0 - fr[spot, :]) * near + fw[spot, :] * far
        out[pl.ds(base * FIELD + j, count, stride=ROWS), :] = value

    complete(OZ)

    def ozone_row(j, carry):
        advect(j, oz, LEV, 7)
        return carry

    lax.fori_loop(0, ROWS, ozone_row, 0)

    def step(k, carry):
        @pl.when(k < NB)
        def _():
            forward(k)

        @pl.when(jnp.logical_and(k >= LAG_B, k < NB + LAG_B))
        def _():
            forward_relayed(k - LAG_B)

        @pl.when(k >= LAG_C)
        def _():
            complete(k - LAG_C)
            for r in range(CH):
                advect((k - LAG_C) * CH + r, qb, 4 * LEV, 3)

        return carry

    lax.fori_loop(0, NB + LAG_C, step, 0)

    all_edges(lambda copy: copy.wait_send())
    for ch in range(NCH):

        @pl.when(lat > 0)
        def _():
            row_copy(0, ch).wait_send()

        @pl.when(lat < N_LAT - 1)
        def _():
            row_copy(1, ch).wait_send()

    drain(OZ)

    def drain_block(n, carry):
        drain(n)
        return carry

    lax.fori_loop(0, NB, drain_block, 0)


def place(state, flux, state_out, flux_out, sem):
    copies = [pltpu.make_async_copy(flux, flux_out, sem.at[4])]
    for part in range(4):
        spot = slice(part * 2 * FIELD, (part + 1) * 2 * FIELD)
        copies.append(pltpu.make_async_copy(state.at[spot], state_out.at[spot], sem.at[part]))
    for copy in copies:
        copy.start()
    for copy in copies:
        copy.wait()


def on_device(state, surface, layer_one, layer_two, layer_three, layer_four, layer_five, lit_columns, row_offset):
    fields = state.shape[0]
    any_spec = pl.BlockSpec(memory_space=pl.ANY)
    vmem_spec = pl.BlockSpec(memory_space=pltpu.VMEM)
    dma = pltpu.SemaphoreType.DMA
    new_state, surface_flux = pl.pallas_call(
        kernel,
        out_shape=(
            pltpu.VMEM((fields * FIELD + SPARE, COLS), F32),
            pltpu.VMEM((8 * ROWS, COLS), BF16),
        ),
        in_specs=[any_spec] * 8 + [pl.BlockSpec(memory_space=pltpu.SMEM)],
        out_specs=(vmem_spec, vmem_spec),
        scratch_shapes=[
            pltpu.VMEM((fields * FIELD + SPARE, COLS), F32),
            pltpu.VMEM((76 * ROWS, COLS), BF16),
            pltpu.VMEM((76 * ROWS + SPARE, COLS), F32),
            pltpu.VMEM((NIN, H1), BF16),
            pltpu.VMEM((H1, H2), BF16),
            pltpu.VMEM((H2, H3), BF16),
            pltpu.VMEM((H3, H4), BF16),
            pltpu.VMEM((NOUT, H4), BF16),
            pltpu.VMEM((ROWS, COLS), jnp.int32),
            pltpu.VMEM((ROWS * COLS, H1), F32),
            pltpu.VMEM((2 * ROWS, COLS), F32),
            pltpu.VMEM((4 * FIELD, COLS), F32),
            pltpu.VMEM((4 * FIELD, COLS), F32),
            pltpu.VMEM((8 * ROWS, COLS), F32),
            pltpu.VMEM((FIELD, COLS), F32),
            pltpu.VMEM((2, NCH, LC * ROWS, COLS), BF16),
            pltpu.VMEM((2, NCH, LC * ROWS, COLS), BF16),
            pltpu.VMEM((EROWS, COLS), F32),
            pltpu.VMEM((EROWS, COLS), BF16),
            pltpu.VMEM((2, EROWS // 2, COLS), BF16),
            pltpu.VMEM((2, EROWS, COLS), BF16),
            pltpu.VMEM((6, EROWS // 2, COLS), BF16),
            pltpu.VMEM((10, GROUPS * ROWS, COLS), F32),
            pltpu.VMEM((5, ROWS, LEV, COLS), BF16),
            pltpu.VMEM((5, ROWS, 4 * LEV, COLS), BF16),
            dma((9,)),
            dma((2, NCH)),
            dma((2, NCH)),
            dma((8,)),
            dma((8,)),
            dma((NB + 1, 5)),
            dma((NB + 1, 5)),
        ],
        compiler_params=pltpu.CompilerParams(
            collective_id=0, has_side_effects=True, vmem_limit_bytes=56 * 1024 * 1024
        ),
    )(
        state.reshape(fields * FIELD, COLS),
        surface.reshape(76 * ROWS, COLS),
        layer_one, layer_two, layer_three, layer_four, layer_five.T,
        lit_columns.reshape(ROWS, COLS),
        row_offset,
    )
    new_state, surface_flux = pl.pallas_call(
        place,
        out_shape=(
            jax.ShapeDtypeStruct((fields * FIELD, COLS), F32),
            jax.ShapeDtypeStruct((8 * ROWS, COLS), BF16),
        ),
        in_specs=[vmem_spec, vmem_spec],
        out_specs=(any_spec, any_spec),
        scratch_shapes=[dma((5,))],
    )(pltpu.with_memory_space_constraint(new_state, pltpu.VMEM), pltpu.with_memory_space_constraint(surface_flux, pltpu.VMEM))
    return new_state.reshape(fields, LEV, ROWS, COLS), surface_flux.reshape(8, ROWS, COLS)


def solution(mesh):
    in_specs = (
        P(None, None, "lat", "lon"), P(None, "lat", "lon"), P(), P(), P(), P(), P(), P("lat", "lon", None), P("lat"),
    )
    out_specs = (P(None, None, "lat", "lon"), P(None, "lat", "lon"))
    return jax.shard_map(on_device, mesh=mesh, in_specs=in_specs, out_specs=out_specs, check_vma=False)
```
